32 devices in a mesh: groups: 2 (over y), gx: 4 (over z), gy: 4 (over x, core).
Axes of the slice: x: 2, y: 2, z: 4, core: 2. Of those that a mesh axis runs over, the one named last changes fastest.
Arguments:
- tokens: bfloat16 [2, 16, 16384], P(None, 'groups', 'gx'), parts along dimension 1, may hold values from -20 to 20, as said below
- lengths: int32 [2, 16], P(None, ('groups', 'gx')), parts along dimension 1, may hold values from 1 to 1024, as said below
- norm_gain: bfloat16 [16384], P('gx'), may hold values from 0.5 to 2
- w_query: bfloat16 [16384, 8192], P('gx', 'gy'), may hold values from -1.171875 to 1.171875
- key_value_weight: bfloat16 [16384, 4, 256], P('gx', 'gy'), may hold values from -0.046875 to 0.046875
- w_out: bfloat16 [8192, 16384], P('gy', 'gx'), may hold values from -0.0625 to 0.0625
- cache: bfloat16 [2, 16, 1024, 4, 2, 128], P(None, ('groups', 'gx'), None, 'gy'), parts along dimension 1, may hold values from -16 to 16
Outputs:
- layer_out: bfloat16 [2, 16, 16384], P(None, 'groups', 'gx'), parts along dimension 1
The draws below stay inside these ranges and needn't reach their ends.
There are 2 independent parts, one for each index of `groups`. The reference program is written for one: setup_inputs(seed, part) draws one part's arguments, and reference() takes and returns one part's arrays. A program takes and returns all parts, laid end to end along the dimension named above; an argument that names none is the same for every part. Nothing has to cross between parts.
Inputs may be any that keep to these rules, and one draw needn't show every extreme that they name: `tokens`: entries vary with the feature and the row. `lengths`: some rollout has exactly 1024 cached positions in every draw.
All inputs are finite; a program needn't handle non-finite values.
Results may differ from the reference program's by a relative error of at most 0.012.
The reference program's roundings to bfloat16 on the way count: a program that leaves them out, or rounds other values in their place, can miss the bound.
Values may be sent and summed in bfloat16 or wider, within the bound.
A program may use at most 128 MiB of HBM per device.

```python
import math
import jax
import jax.numpy as jnp
from jax import lax

MODEL_WIDTH = 16384
QUERY_HEADS = 64
KEY_VALUE_HEADS = 4
HEAD_SIZE = 128
MICRO_BATCHES = 2
CACHE_POSITIONS = 1024
BATCH_ROLLOUTS = 8


def draw_tokens(key, part):
    first = jax.random.fold_in(key, 0)
    columns = jnp.exp(jnp.linspace(jnp.log(0.5), jnp.log(1.5), MODEL_WIDTH)).astype(jnp.float32)
    base = jax.random.truncated_normal(first, -6.0, 6.0, (MICRO_BATCHES, BATCH_ROLLOUTS, MODEL_WIDTH), jnp.float32)
    return (base * columns).astype(jnp.bfloat16)


def draw_lengths(key, part):
    counts = jax.random.randint(key, (MICRO_BATCHES, BATCH_ROLLOUTS), 1, CACHE_POSITIONS + 1, dtype=jnp.int32)
    return counts.at[0, 0].set(CACHE_POSITIONS)


def draw_w_query(key, part):
    first = jax.random.fold_in(jax.random.fold_in(key, 7), 0)
    base = jax.random.truncated_normal(first, -6.0, 6.0, (MODEL_WIDTH, QUERY_HEADS * HEAD_SIZE), jnp.float32) * MODEL_WIDTH ** (-0.5)
    return base.astype(jnp.bfloat16)


def draw_cache(key, part):
    factor = jnp.array([2.5, 1.0], dtype=jnp.float32).reshape(1, 1, 1, 1, 2, 1)
    array_shape = (MICRO_BATCHES, BATCH_ROLLOUTS, CACHE_POSITIONS, KEY_VALUE_HEADS, 2, HEAD_SIZE)
    base = jax.random.truncated_normal(key, -6.0, 6.0, array_shape, jnp.float32)
    return (base * factor).astype(jnp.bfloat16)


def block_levels(key, extent, cuts, low, largest):
    gain, own = 1.0, jax.random.fold_in(key, 6)
    for dim, shards_of in cuts:
        draws = jnp.exp(jax.random.uniform(jax.random.fold_in(own, dim), (shards_of,), jnp.float32, low / len(cuts), largest / len(cuts)))
        gain = gain * jnp.repeat(draws, extent[dim] // shards_of).reshape([-1 if axis == dim else 1 for axis in range(len(extent))])
    return gain


def scatter_about(own_key, shape, width, reach, cuts=(), held_as=jnp.bfloat16):
    drawn = jax.random.normal(own_key, shape, jnp.float32) * width
    if len(cuts) > 0:
        drawn = block_levels(own_key, shape, cuts, -0.22, 0.18) * drawn
    return jnp.clip(drawn, min=-reach, max=reach).astype(held_as)


def setup_inputs(seed: int = 0, part: int = 0) -> dict:
    arg_keys = jax.random.split(jax.random.key(seed), 8)
    own_keys = jax.random.split(jax.random.fold_in(arg_keys[7], part), 8)
    return {
        "tokens": draw_tokens(jax.random.fold_in(jax.random.fold_in(arg_keys[7], part), 71), part),
        "lengths": draw_lengths(jax.random.fold_in(jax.random.fold_in(arg_keys[7], part), 71), part),
        "norm_gain": jnp.clip(jnp.exp(math.log(2.0) - 1.3862944 * jax.random.uniform(arg_keys[2], (MODEL_WIDTH,), jnp.float32) ** block_levels(arg_keys[2], (MODEL_WIDTH,), ((0, 4),), -0.2, 0.2)), 0.5, 2.0).astype(jnp.bfloat16),
        "w_query": draw_w_query(jax.random.fold_in(arg_keys[7], 71), part),
        "key_value_weight": scatter_about(arg_keys[4], (MODEL_WIDTH, KEY_VALUE_HEADS, 2 * HEAD_SIZE), MODEL_WIDTH ** -0.5, 0.046875, ((0, 4), (1, 4))),
        "w_out": scatter_about(arg_keys[5], (QUERY_HEADS * HEAD_SIZE, MODEL_WIDTH), (QUERY_HEADS * HEAD_SIZE) ** -0.5, 0.0625, ((0, 4), (1, 4))),
        "cache": draw_cache(jax.random.fold_in(jax.random.fold_in(arg_keys[7], part), 71), part),
    }


def rotate(vectors, positions):
    half = vectors.shape[-1] // 2
    freq = 500000.0 ** (-2.0 * jnp.arange(half, dtype=jnp.float32) / vectors.shape[-1])
    angle = positions[..., None] * freq
    cosine = jnp.cos(angle)
    sine = jnp.sin(angle)
    first = vectors[..., :half]
    second = vectors[..., half:]
    return jnp.concatenate([first * cosine - second * sine, second * cosine + first * sine], axis=-1)

def reference(tokens, lengths, norm_gain, w_query, key_value_weight, w_out, cache):
    x_full = tokens.astype(jnp.float32)
    score_scale = lax.rsqrt(lax.optimization_barrier(jnp.mean(x_full * x_full, axis=-1)) + 1e-05)
    normed = (x_full * norm_gain.astype(jnp.float32)).astype(jnp.bfloat16)
    flattened = normed.reshape(MICRO_BATCHES * BATCH_ROLLOUTS, MODEL_WIDTH)
    query = jnp.dot(flattened, w_query, preferred_element_type=jnp.float32).reshape(MICRO_BATCHES, BATCH_ROLLOUTS, QUERY_HEADS, HEAD_SIZE)
    query = query * score_scale[:, :, None, None]
    key_value = jnp.dot(flattened, key_value_weight.reshape(MODEL_WIDTH, KEY_VALUE_HEADS * 2 * HEAD_SIZE), preferred_element_type=jnp.float32)
    key_value = key_value.reshape(MICRO_BATCHES, BATCH_ROLLOUTS, KEY_VALUE_HEADS, 2 * HEAD_SIZE) * score_scale[:, :, None, None]
    positions = lengths.astype(jnp.float32)[:, :, None]
    rotated_query = rotate(query, positions).astype(jnp.bfloat16)
    rkey = rotate(key_value[..., :HEAD_SIZE], positions)
    value_new = key_value[..., HEAD_SIZE:]
    query_group = QUERY_HEADS // KEY_VALUE_HEADS
    group_queries = rotated_query.reshape(MICRO_BATCHES, BATCH_ROLLOUTS, KEY_VALUE_HEADS, query_group, HEAD_SIZE)
    inv_root = 1.0 / jnp.sqrt(jnp.float32(HEAD_SIZE))

    def one_batch(items):
        qpart, kpart, vpart, cpart, lpart = items
        keys = cpart[:, :, :, 0, :].astype(jnp.float32)
        values = cpart[:, :, :, 1, :].astype(jnp.float32)
        qfull = qpart.astype(jnp.float32)
        scores = jnp.einsum('rkgd,rskd->rkgs', qfull, keys, precision=lax.Precision.HIGHEST) * inv_root
        valid = jnp.arange(CACHE_POSITIONS, dtype=jnp.int32)[None, :] < lpart[:, None]
        scores = jnp.where(valid[:, None, None, :], scores, -1e+30)
        new_score = lax.optimization_barrier(jnp.sum(qfull * kpart[:, :, None, :], axis=-1)) * inv_root
        top = jnp.maximum(lax.optimization_barrier(jnp.max(scores, axis=-1)), new_score)
        weights = jnp.exp(scores - top[..., None])
        new_weight = jnp.exp(new_score - top)
        total = lax.optimization_barrier(jnp.sum(weights, axis=-1)) + new_weight
        bweights = weights.astype(jnp.bfloat16).astype(jnp.float32)
        summed = jnp.einsum('rkgs,rskd->rkgd', bweights, values, precision=lax.Precision.HIGHEST)
        summed = summed + new_weight[..., None] * vpart[:, :, None, :]
        return (summed / total[..., None]).astype(jnp.bfloat16)
    attended = lax.map(one_batch, (group_queries, rkey, value_new, cache, lengths))
    attended = attended.reshape(MICRO_BATCHES * BATCH_ROLLOUTS, QUERY_HEADS * HEAD_SIZE)
    projected = jnp.dot(attended, w_out, preferred_element_type=jnp.float32).reshape(MICRO_BATCHES, BATCH_ROLLOUTS, MODEL_WIDTH)
    return (x_full + projected).astype(jnp.bfloat16)
```

```python
import functools

import jax
import jax.numpy as jnp
import numpy as np
from jax import lax
from jax.experimental import pallas as pl
from jax.experimental.pallas import tpu as pltpu
from jax.sharding import PartitionSpec as P

MODEL_WIDTH = 16384
HEAD_SIZE = 128
ROPE_BASE = 500000.0
MESH = pl.DeviceIdType.MESH


def kernel(
    n, ny, hc, splits, o_chunk,
    lens_hbm, tok_hbm, gain_hbm, freq_hbm, wq_hbm, wk_hbm, wo_hbm, kv_hbm,
    out,
    lens, tok, gain, freq, wq, wk, wo, kv, normed,
    send, recv, tail_send, tail_recv, att_send, att_recv, x_f, x_s,
    ybuf, fold_s, fold_r, cross_s, cross_r,
    small_sem, wq_sem, wk_sem, wo_sem, kv_sem,
    qs_sem, qr_sem, as_sem, ar_sem, fs_sem, fr_sem, cs_sem, cr_sem, os_sem, or_sem,
):
    batches, rows, depth = tok.shape
    here = rows // n
    total_rows = batches * rows
    q_width = wq.shape[1]
    kv_width = wk.shape[1]
    heads = q_width // HEAD_SIZE
    out_width = wo.shape[1]
    nq = heads // hc
    no = out_width // o_chunk
    local_rows = batches * here
    pairs = local_rows // 2
    positions = kv.shape[1]
    q_chunk = hc * HEAD_SIZE
    k_part = depth // splits
    bits = ny.bit_length() - 1
    me = lax.axis_index("gx")
    my = lax.axis_index("gy")
    leader = lax.rem(my, 2) == 1
    follower = lax.rem(my, 2) == 0

    smalls = [
        pltpu.make_async_copy(tok_hbm, tok, small_sem.at[0]),
        pltpu.make_async_copy(gain_hbm, gain, small_sem.at[1]),
        pltpu.make_async_copy(freq_hbm, freq, small_sem.at[2]),
        pltpu.make_async_copy(lens_hbm, lens, small_sem.at[3]),
    ]

    def wq_copy(c, k):
        at = (pl.ds(k * k_part, k_part), pl.ds(c * q_chunk, q_chunk))
        return pltpu.make_async_copy(wq_hbm.at[at], wq.at[at], wq_sem.at[c, k])

    def wo_copy(c):
        at = pl.ds(c * q_chunk, q_chunk)
        return pltpu.make_async_copy(wo_hbm.at[at], wo.at[at], wo_sem.at[c])

    def kv_copy(r):
        return pltpu.make_async_copy(
            kv_hbm.at[pl.ds(r * positions, positions)],
            kv.at[r // 2, :, pl.ds((r % 2) * HEAD_SIZE, HEAD_SIZE)],
            kv_sem.at[r],
        )

    for copy in smalls:
        copy.start()
    wk_copy = pltpu.make_async_copy(wk_hbm, wk, wk_sem)
    wk_copy.start()
    for c in range(nq):
        for k in range(splits):
            wq_copy(c, k).start()
    for r in range(local_rows):
        kv_copy(r).start()
    for c in range(nq):
        wo_copy(c).start()

    barrier = pltpu.get_barrier_semaphore()

    def each(fn):
        if n <= 8:
            for d in range(1, n):
                fn(d)
        else:
            def body(d, carry):
                fn(d)
                return carry
            lax.fori_loop(1, n, body, 0)

    def greet(d):
        pl.semaphore_signal(
            barrier, inc=1, device_id={"gx": lax.rem(me + d, n)}, device_id_type=MESH
        )

    each(greet)

    def across(level):
        step = 1 << level
        return my + step - 2 * step * lax.rem(my // step, 2)

    for level in range(bits):
        pl.semaphore_signal(barrier, inc=1, device_id={"gy": across(level)}, device_id_type=MESH)

    for copy in smalls:
        copy.wait()
    x = tok[...].astype(jnp.float32).reshape(total_rows, depth)
    for k in range(depth // HEAD_SIZE):
        cols = slice(k * HEAD_SIZE, (k + 1) * HEAD_SIZE)
        normed[:, cols] = (x[:, cols] * gain[k:k + 1, :].astype(jnp.float32)).astype(jnp.bfloat16)
    squares = jnp.broadcast_to(jnp.sum(x * x, axis=1, keepdims=True), (total_rows, HEAD_SIZE))

    def to(d):
        return lax.rem(me + d, n)

    def source(d):
        return lax.rem(me - d + n, n)

    def shift(c, d, peer):
        src, dst = (tail_send, tail_recv) if c == nq else (send.at[c], recv.at[c])
        return pltpu.make_async_remote_copy(
            src_ref=src.at[to(d)],
            dst_ref=dst.at[peer],
            send_sem=qs_sem.at[c, d],
            recv_sem=qr_sem.at[c, d],
            device_id={"gx": to(d)},
            device_id_type=MESH,
        )

    wk_copy.wait()
    keyval = jnp.dot(normed[...], wk[...], preferred_element_type=jnp.float32)
    for j in range(n):
        for b in range(batches):
            at = slice(b * rows + j * here, b * rows + (j + 1) * here)
            to_at = slice(b * here, (b + 1) * here)
            tail_send[j, to_at, :kv_width] = keyval[at]
            tail_send[j, to_at, kv_width:] = squares[at]
    pl.semaphore_wait(barrier, n - 1 + bits)
    each(lambda d: shift(nq, d, me).start())

    group = local_rows * hc
    for c in range(nq):
        part = None
        for k in range(splits):
            wq_copy(c, k).wait()
            ks = slice(k * k_part, (k + 1) * k_part)
            piece = jnp.dot(
                normed[:, ks], wq[ks, c * q_chunk:(c + 1) * q_chunk],
                preferred_element_type=jnp.float32,
            )
            part = piece if part is None else part + piece
        for j in range(n):
            for b in range(batches):
                at = slice(b * rows + j * here, b * rows + (j + 1) * here)
                for h in range(hc):
                    send[c, j, pl.ds(b * here * hc + h, here, stride=hc), :] = part[
                        at, h * HEAD_SIZE:(h + 1) * HEAD_SIZE
                    ]
        each(lambda d: shift(c, d, me).start())

    lane = lax.broadcasted_iota(jnp.int32, (group, HEAD_SIZE), 1)
    owner = lax.broadcasted_iota(jnp.int32, (group, HEAD_SIZE), 0) // hc
    place = jnp.zeros((group, HEAD_SIZE), jnp.float32)
    for r in range(local_rows):
        place = jnp.where(owner == r, lens[r // here, r % here].astype(jnp.float32), place)
    angle = place * freq[...]
    cosine = jnp.cos(angle)
    sine = jnp.sin(angle)
    sine = jnp.where(lane < HEAD_SIZE // 2, -sine, sine)

    def rotate(v):
        return v * cosine + pltpu.roll(v, HEAD_SIZE // 2, 1) * sine

    def wait_from(c):
        each(lambda d: shift(c, d, source(d)).wait_recv())

    def summed(mine, theirs):
        def add(d, acc):
            return acc + theirs[to(d)]
        return lax.fori_loop(1, n, add, mine[me], unroll=n <= 8)

    wait_from(nq)
    tail = summed(tail_send, tail_recv)

    def spread_rows(v):
        return jnp.concatenate(
            [jnp.broadcast_to(v[r:r + 1], (hc, v.shape[1])) for r in range(local_rows)], axis=0
        )

    scale = lax.rsqrt(spread_rows(tail[:, kv_width:]) / MODEL_WIDTH + 1e-05)
    rkey = rotate(spread_rows(tail[:, :HEAD_SIZE]) * scale)
    value_new = spread_rows(tail[:, HEAD_SIZE:2 * HEAD_SIZE]) * scale

    inv_root = np.float32(1.0 / np.sqrt(np.float32(HEAD_SIZE)))
    column = lax.broadcasted_iota(jnp.int32, (2 * hc, positions), 1)
    key_column = jnp.where(lax.rem(column, 2) == 0, column, 2 * positions)
    first = lax.broadcasted_iota(jnp.int32, (2 * hc, HEAD_SIZE), 0) < hc
    first_wide = lax.broadcasted_iota(jnp.int32, (2 * hc, positions), 0) < hc

    def spread(c, d, peer):
        return pltpu.make_async_remote_copy(
            src_ref=att_send.at[c], dst_ref=att_recv.at[c, peer],
            send_sem=as_sem.at[c, d], recv_sem=ar_sem.at[c, d],
            device_id={"gx": to(d)}, device_id_type=MESH,
        )

    for c in range(nq):
        wait_from(c)
        rquery = rotate(summed(send.at[c], recv.at[c]) * scale).astype(jnp.bfloat16)
        rquery = rquery.astype(jnp.float32)
        new_scores = jnp.sum(rquery * rkey, axis=1, keepdims=True) * inv_root
        done = []
        for p in range(pairs):
            if c == 0:
                kv_copy(2 * p).wait()
                kv_copy(2 * p + 1).wait()
            at = slice(p * 2 * hc, (p + 1) * 2 * hc)
            query = rquery[at]
            both = jnp.concatenate(
                [jnp.where(first, query, 0.0), jnp.where(first, 0.0, query)], axis=1
            ).astype(jnp.bfloat16)
            scores = (
                lax.dot_general(
                    both, kv[p], (((1,), (1,)), ((), ())), preferred_element_type=jnp.float32
                )
                * inv_root
            )
            r = 2 * p
            limit = jnp.where(
                first_wide, 2 * lens[r // here, r % here],
                2 * lens[(r + 1) // here, (r + 1) % here],
            )
            scores = jnp.where(key_column < limit, scores, -1e30)
            new_score = new_scores[at]
            top = jnp.maximum(jnp.max(scores, axis=1, keepdims=True), new_score)
            weights = jnp.exp(scores - top)
            new_weight = jnp.exp(new_score - top)
            total = jnp.sum(weights, axis=1, keepdims=True) + new_weight
            moved = pltpu.roll(weights, 1, 1).astype(jnp.bfloat16)
            mixed = jnp.dot(moved, kv[p], preferred_element_type=jnp.float32)
            mixed = jnp.where(first, mixed[:, :HEAD_SIZE], mixed[:, HEAD_SIZE:])
            done.append((mixed + new_weight * value_new[at]) / total)
        attended = jnp.concatenate(done, axis=0).astype(jnp.bfloat16)
        att_send[c] = attended
        att_recv[c, me] = attended
        each(lambda d: spread(c, d, me).start())

    def fold(o):
        cols = pl.ds(o * o_chunk, o_chunk)
        return pltpu.make_async_remote_copy(
            src_ref=fold_s.at[:, cols], dst_ref=fold_r.at[:, cols],
            send_sem=fs_sem.at[o], recv_sem=fr_sem.at[o],
            device_id={"gy": across(0)}, device_id_type=MESH,
        )

    def cross(o, k):
        cols = pl.ds(o * o_chunk, o_chunk)
        return pltpu.make_async_remote_copy(
            src_ref=cross_s.at[k, :, cols], dst_ref=cross_r.at[k, :, cols],
            send_sem=cs_sem.at[k, o], recv_sem=cr_sem.at[k, o],
            device_id={"gy": across(k + 1)}, device_id_type=MESH,
        )

    def give(o):
        cols = pl.ds(o * o_chunk, o_chunk)
        return pltpu.make_async_remote_copy(
            src_ref=out.at[:, :, cols], dst_ref=out.at[:, :, cols],
            send_sem=os_sem.at[o], recv_sem=or_sem.at[o],
            device_id={"gy": across(0)}, device_id_type=MESH,
        )

    for c in range(nq):
        each(lambda d: spread(c, d, source(d)).wait_recv())
        x_f[...] = att_recv[c].astype(jnp.float32).reshape(n * group, HEAD_SIZE)
        for j in range(n):
            for b in range(batches):
                at = slice(b * rows + j * here, b * rows + (j + 1) * here)
                for h in range(hc):
                    x_s[at, h * HEAD_SIZE:(h + 1) * HEAD_SIZE] = x_f[
                        pl.ds(j * group + b * here * hc + h, here, stride=hc), :
                    ]
        xc = x_s[...].astype(jnp.bfloat16)
        wo_copy(c).wait()
        for o in range(no):
            cols = slice(o * o_chunk, (o + 1) * o_chunk)
            y = jnp.dot(
                xc, wo[c * q_chunk:(c + 1) * q_chunk, cols], preferred_element_type=jnp.float32
            )
            if c > 0:
                y = y + ybuf[:, cols]
            ybuf[:, cols] = y
            if c == nq - 1:
                @pl.when(follower)
                def _(o=o, cols=cols, y=y):
                    fold_s[:, cols] = y.astype(jnp.bfloat16)
                    fold(o).start()

    @pl.when(leader)
    def _():
        for o in range(no):
            cols = slice(o * o_chunk, (o + 1) * o_chunk)
            fold(o).wait_recv()
            y = ybuf[:, cols] + fold_r[:, cols].astype(jnp.float32)
            if bits > 1:
                cross_s[0, :, cols] = y.astype(jnp.bfloat16)
                cross(o, 0).start()
            else:
                ybuf[:, cols] = y
        for k in range(bits - 1):
            for o in range(no):
                cols = slice(o * o_chunk, (o + 1) * o_chunk)
                cross(o, k).wait_recv()
                y = cross_s[k, :, cols].astype(jnp.float32) + cross_r[k, :, cols].astype(jnp.float32)
                if k < bits - 2:
                    cross_s[k + 1, :, cols] = y.astype(jnp.bfloat16)
                    cross(o, k + 1).start()
                else:
                    y = y.reshape(batches, rows, o_chunk)
                    out[:, :, cols] = (tok[:, :, cols].astype(jnp.float32) + y).astype(jnp.bfloat16)
                    give(o).start()
        for o in range(no):
            for k in range(bits - 1):
                cross(o, k).wait_send()
            give(o).wait_send()

    @pl.when(follower)
    def _():
        for o in range(no):
            fold(o).wait_send()
        for o in range(no):
            give(o).wait_recv()

    for c in range(nq + 1):
        each(lambda d: shift(c, d, me).wait_send())
    for c in range(nq):
        each(lambda d: spread(c, d, me).wait_send())


def local(n, ny, tokens, lengths, norm_gain, w_query, key_value_weight, w_out, cache):
    batches, rows, depth = tokens.shape
    here = rows // n
    local_rows = batches * here
    q_width = w_query.shape[1]
    kv_heads = key_value_weight.shape[1]
    kv_width = kv_heads * key_value_weight.shape[2]
    assert kv_heads == 1 and ny >= 4 and ny & (ny - 1) == 0 and local_rows % 2 == 0
    heads = q_width // HEAD_SIZE
    out_width = w_out.shape[1]
    hc = 4
    splits = 2 if depth % 4096 == 0 else 1
    o_chunk = min(1024, out_width)
    nq, no = heads // hc, out_width // o_chunk
    assert nq * hc == heads
    bits = ny.bit_length() - 1
    freq = np.float32(ROPE_BASE) ** (
        -2.0 * np.arange(HEAD_SIZE // 2, dtype=np.float32) / HEAD_SIZE
    )
    freq = np.concatenate([freq, freq]).astype(np.float32)[None, :]
    positions = cache.shape[2] * 2
    interleaved = cache.reshape(local_rows * positions, HEAD_SIZE)
    hbm = pl.BlockSpec(memory_space=pltpu.HBM)
    f32, bf16 = jnp.float32, jnp.bfloat16
    dma = pltpu.SemaphoreType.DMA
    total_rows = batches * rows
    group = local_rows * hc
    return pl.pallas_call(
        functools.partial(kernel, n, ny, hc, splits, o_chunk),
        out_shape=pltpu.VMEM(tokens.shape, bf16),
        in_specs=[hbm] * 8,
        out_specs=pl.BlockSpec(memory_space=pltpu.VMEM),
        scratch_shapes=[
            pltpu.SMEM(lengths.shape, jnp.int32),
            pltpu.VMEM(tokens.shape, bf16),
            pltpu.VMEM((depth // HEAD_SIZE, HEAD_SIZE), bf16),
            pltpu.VMEM((1, HEAD_SIZE), f32),
            pltpu.VMEM(w_query.shape, bf16),
            pltpu.VMEM((depth, kv_width), bf16),
            pltpu.VMEM(w_out.shape, bf16),
            pltpu.VMEM((local_rows // 2, positions, 2 * HEAD_SIZE), bf16),
            pltpu.VMEM((total_rows, depth), bf16),
            pltpu.VMEM((nq, n, group, HEAD_SIZE), f32),
            pltpu.VMEM((nq, n, group, HEAD_SIZE), f32),
            pltpu.VMEM((n, local_rows, kv_width + HEAD_SIZE), f32),
            pltpu.VMEM((n, local_rows, kv_width + HEAD_SIZE), f32),
            pltpu.VMEM((nq, group, HEAD_SIZE), bf16),
            pltpu.VMEM((nq, n, group, HEAD_SIZE), bf16),
            pltpu.VMEM((n * group, HEAD_SIZE), f32),
            pltpu.VMEM((total_rows, hc * HEAD_SIZE), f32),
            pltpu.VMEM((total_rows, out_width), f32),
            pltpu.VMEM((total_rows, out_width), bf16),
            pltpu.VMEM((total_rows, out_width), bf16),
            pltpu.VMEM((bits - 1, total_rows, out_width), bf16),
            pltpu.VMEM((bits - 1, total_rows, out_width), bf16),
            dma((4,)), dma((nq, splits)), dma, dma((nq,)), dma((local_rows,)),
            dma((nq + 1, n)), dma((nq + 1, n)), dma((nq, n)), dma((nq, n)),
            dma((no,)), dma((no,)), dma((bits - 1, no)), dma((bits - 1, no)),
            dma((no,)), dma((no,)),
        ],
        compiler_params=pltpu.CompilerParams(
            collective_id=0, has_side_effects=True, vmem_limit_bytes=67043328 - 2 * tokens.size
        ),
    )(
        lengths, tokens, norm_gain.reshape(depth // HEAD_SIZE, HEAD_SIZE), jnp.asarray(freq),
        w_query, key_value_weight.reshape(depth, kv_width), w_out, interleaved,
    )


def solution(mesh):
    placed = (
        P(None, "groups", "gx"),
        P(None, ("groups", "gx")),
        P("gx"),
        P("gx", "gy"),
        P("gx", "gy", None),
        P("gy", "gx"),
        P(None, ("groups", "gx"), None, "gy", None, None),
    )
    return jax.shard_map(
        functools.partial(local, mesh.shape["gx"], mesh.shape["gy"]),
        mesh=mesh, in_specs=placed, out_specs=P(None, "groups", "gx"), check_vma=False,
    )
```

```python
import functools

import jax
import jax.numpy as jnp
import numpy as np
from jax import lax
from jax.experimental import pallas as pl
from jax.experimental.pallas import tpu as pltpu
from jax.sharding import PartitionSpec as P

MODEL_WIDTH = 16384
HEAD_SIZE = 128
ROPE_BASE = 500000.0
MESH = pl.DeviceIdType.MESH


def kernel(
    n, ny, chunks, splits, phases, ahead, outs,
    lens_hbm, tok_hbm, gain_hbm, freq_hbm, wq_hbm, wk_hbm, wo_hbm, kv_hbm,
    out,
    lens, tok, gain, freq, wq, wk, wo, kv, normed,
    acc, wide_s, keys, values, send, recv, q_s, o_s, att_send, att_recv, x_s,
    ybuf, y_send, y_recv,
    small_sem, stream_sem, wo_sem, kv_sem,
    qs_sem, qr_sem, as_sem, ar_sem, ys_sem, yr_sem, os_sem, or_sem,
):
    batches, rows, depth = tok.shape
    here = rows // n
    total_rows = batches * rows
    q_width = wq.shape[1]
    kv_width = wk.shape[1]
    out_width = wo.shape[1]
    local_rows = batches * here
    pairs = local_rows // 2
    positions = keys.shape[1]
    last = len(phases) - 1
    starts = [sum(phases[:i]) * HEAD_SIZE for i in range(len(phases))]
    widths = [heads * HEAD_SIZE for heads in phases]
    nc = len(chunks)
    q_starts = [sum(chunks[:i]) * HEAD_SIZE for i in range(nc)]
    q_widths = [heads * HEAD_SIZE for heads in chunks]
    me = lax.axis_index("gx")
    my = lax.axis_index("gy")
    leader = lax.rem(my, 2) == 1
    follower = lax.rem(my, 2) == 0

    small = [
        pltpu.make_async_copy(tok_hbm, tok, small_sem.at[0]),
        pltpu.make_async_copy(gain_hbm, gain, small_sem.at[1]),
        pltpu.make_async_copy(freq_hbm, freq, small_sem.at[2]),
        pltpu.make_async_copy(lens_hbm, lens, small_sem.at[3]),
    ]

    pieces = [(wk_hbm, wk)]
    for c in range(nc):
        part = depth // splits[c]
        for k in range(splits[c]):
            at = (pl.ds(k * part, part), pl.ds(q_starts[c], q_widths[c]))
            pieces.append((wq_hbm.at[at], wq.at[at]))

    def stream(i):
        return pltpu.make_async_copy(*pieces[i], stream_sem.at[i % ahead])

    kv_copy = pltpu.make_async_copy(kv_hbm, kv, kv_sem)

    def take(i):
        stream(i).wait()
        if i + ahead < len(pieces):
            stream(i + ahead).start()
        elif i + ahead == len(pieces):
            kv_copy.start()

    def wo_copy(c):
        at = pl.ds(starts[c], widths[c])
        return pltpu.make_async_copy(wo_hbm.at[at], wo.at[at], wo_sem.at[c])

    for copy in small:
        copy.start()
    for i in range(ahead):
        stream(i).start()

    barrier = pltpu.get_barrier_semaphore()

    def each(fn):
        if n <= 8:
            for d in range(1, n):
                fn(d)
        else:
            def body(d, carry):
                fn(d)
                return carry
            lax.fori_loop(1, n, body, 0)

    def greet(d):
        pl.semaphore_signal(
            barrier, inc=1, device_id={"gx": lax.rem(me + d, n)}, device_id_type=MESH
        )

    each(greet)

    for d in range(1, ny):
        pl.semaphore_signal(
            barrier, inc=1, device_id={"gy": lax.rem(my + d, ny)}, device_id_type=MESH
        )

    def to(d):
        return lax.rem(me + d, n)

    def drain(ref, sem):
        pltpu.make_async_copy(ref, ref, sem).wait()

    small[0].wait()
    small[1].wait()
    x = tok[...].astype(jnp.float32).reshape(total_rows, depth)
    for k in range(depth // HEAD_SIZE):
        cols = slice(k * HEAD_SIZE, (k + 1) * HEAD_SIZE)
        normed[:, cols] = (x[:, cols] * gain[k:k + 1, :].astype(jnp.float32)).astype(jnp.bfloat16)
    squares = jnp.broadcast_to(jnp.sum(x * x, axis=1, keepdims=True), (total_rows, HEAD_SIZE))

    def put(part, start):
        width = part.shape[1]
        for j in range(n):
            for b in range(batches):
                send[j, b * here:(b + 1) * here, start:start + width] = part[
                    b * rows + j * here:b * rows + (j + 1) * here, :
                ]

    def shift(c, start, width):
        cols = pl.ds(start, width)
        def one(d):
            pltpu.make_async_remote_copy(
                src_ref=send.at[to(d), :, cols], dst_ref=recv.at[me, :, cols],
                send_sem=qs_sem, recv_sem=qr_sem.at[c],
                device_id={"gx": to(d)}, device_id_type=MESH,
            ).start()
        each(one)

    def arrived(c, start, width):
        drain(recv.at[pl.ds(0, n - 1), :, pl.ds(start, width)], qr_sem.at[c])

    def summed(start, width):
        cols = pl.ds(start, width)
        def add(d, acc):
            return acc + recv[to(d), :, cols]
        return lax.fori_loop(1, n, add, send[me, :, cols], unroll=n <= 8)

    side = kv_width + HEAD_SIZE
    take(0)
    middle = depth // 2
    for k in range(2):
        ks = slice(k * middle, (k + 1) * middle)
        acc[:, k * kv_width:(k + 1) * kv_width] = jnp.dot(
            normed[:, ks], wk[ks], preferred_element_type=jnp.float32
        )
    for j in range(n):
        for b in range(batches):
            at = slice(b * rows + j * here, b * rows + (j + 1) * here)
            send[j, b * here:(b + 1) * here, q_width:q_width + kv_width] = (
                acc[at, :kv_width] + acc[at, kv_width:2 * kv_width]
            )
    put(squares, q_width + kv_width)
    i = 1
    for c in range(nc):
        size = depth // splits[c]
        for k in range(splits[c]):
            take(i)
            i += 1
            ks = slice(k * size, (k + 1) * size)
            half = q_widths[c] // 2
            for at in (0, half):
                piece = jnp.dot(
                    normed[:, ks], wq[ks, q_starts[c] + at:q_starts[c] + at + half],
                    preferred_element_type=jnp.float32,
                )
                if k > 0:
                    piece = piece + acc[:, at:at + half]
                if k < splits[c] - 1:
                    acc[:, at:at + half] = piece
                else:
                    put(piece, q_starts[c] + at)
        if c == 0:
            pl.semaphore_wait(barrier, n - 1 + ny - 1)
            shift(nc, q_width, side)
        shift(c, q_starts[c], q_widths[c])

    small[2].wait()
    small[3].wait()
    lane = lax.broadcasted_iota(jnp.int32, (local_rows, HEAD_SIZE), 1)
    row = lax.broadcasted_iota(jnp.int32, (local_rows, HEAD_SIZE), 0)
    place = jnp.zeros((local_rows, HEAD_SIZE), jnp.float32)
    for r in range(local_rows):
        place = jnp.where(row == r, lens[r // here, r % here].astype(jnp.float32), place)
    angle = place * freq[...]
    cosine = jnp.cos(angle)
    sine = jnp.sin(angle)
    sine = jnp.where(lane < HEAD_SIZE // 2, -sine, sine)

    def rotate(v):
        return v * cosine + pltpu.roll(v, HEAD_SIZE // 2, 1) * sine

    kv_copy.wait()
    for c in range(last + 1):
        wo_copy(c).start()
    block_rows = wide_s.shape[0]
    blocks = 2 * positions // block_rows

    def divide(t, carry):
        r = t // blocks
        wide_s[...] = kv[pl.ds(pl.multiple_of(t * block_rows, block_rows), block_rows), :].astype(
            jnp.float32
        )
        half = block_rows // 2
        at = pl.ds(pl.multiple_of(lax.rem(t, blocks) * half, half), half)
        lanes = pl.ds(pl.multiple_of(lax.rem(r, 2) * HEAD_SIZE, HEAD_SIZE), HEAD_SIZE)
        keys[r // 2, at, lanes] = wide_s[pl.ds(0, half, stride=2), :].astype(jnp.bfloat16)
        values[r // 2, at, lanes] = wide_s[pl.ds(1, half, stride=2), :].astype(jnp.bfloat16)
        return carry

    lax.fori_loop(0, local_rows * blocks, divide, 0)

    arrived(nc, q_width, side)
    tail = summed(q_width, side)
    scale = lax.rsqrt(tail[:, kv_width:] / MODEL_WIDTH + 1e-05)
    rkey = rotate(tail[:, :HEAD_SIZE] * scale)
    value_new = tail[:, HEAD_SIZE:2 * HEAD_SIZE] * scale
    inv_root = np.float32(1.0 / np.sqrt(np.float32(HEAD_SIZE)))

    def spread(c):
        cols = pl.ds(starts[c], widths[c])
        def one(d):
            pltpu.make_async_remote_copy(
                src_ref=att_send.at[:, cols], dst_ref=att_recv.at[me, :, cols],
                send_sem=as_sem, recv_sem=ar_sem.at[c],
                device_id={"gx": to(d)}, device_id_type=MESH,
            ).start()
        each(one)

    for c in range(last + 1):
        hc = phases[c]
        for i in range(nc):
            if starts[c] <= q_starts[i] < starts[c] + widths[c]:
                arrived(i, q_starts[i], q_widths[i])
        block = summed(starts[c], widths[c])
        for h in range(hc):
            q_s[pl.ds(h, local_rows, stride=hc), :] = rotate(
                block[:, h * HEAD_SIZE:(h + 1) * HEAD_SIZE] * scale
            )
        column = lax.broadcasted_iota(jnp.int32, (2 * hc, positions), 1)
        first = lax.broadcasted_iota(jnp.int32, (2 * hc, HEAD_SIZE), 0) < hc
        first_wide = lax.broadcasted_iota(jnp.int32, (2 * hc, positions), 0) < hc

        def pair_rows(v, p):
            shape = (2 * hc, v.shape[1])
            return jnp.where(
                first,
                jnp.broadcast_to(v[2 * p:2 * p + 1], shape),
                jnp.broadcast_to(v[2 * p + 1:2 * p + 2], shape),
            )

        weighed = []
        for p in range(pairs):
            query = q_s[p * 2 * hc:(p + 1) * 2 * hc, :].astype(jnp.bfloat16).astype(jnp.float32)
            both = jnp.concatenate(
                [jnp.where(first, query, 0.0), jnp.where(first, 0.0, query)], axis=1
            ).astype(jnp.bfloat16)
            scores = jnp.concatenate(
                [
                    lax.dot_general(
                        both, keys[p, at:at + positions // 2], (((1,), (1,)), ((), ())),
                        preferred_element_type=jnp.float32,
                    )
                    for at in (0, positions // 2)
                ],
                axis=1,
            ) * inv_root
            r = 2 * p
            limit = jnp.where(
                first_wide, lens[r // here, r % here], lens[(r + 1) // here, (r + 1) % here]
            )
            scores = jnp.where(column < limit, scores, -1e30)
            new_score = jnp.sum(query * pair_rows(rkey, p), axis=1, keepdims=True) * inv_root
            top = jnp.maximum(jnp.max(scores, axis=1, keepdims=True), new_score)
            weights = jnp.exp(scores - top)
            new_weight = jnp.exp(new_score - top)
            total = jnp.sum(weights, axis=1, keepdims=True) + new_weight
            weighed.append((weights.astype(jnp.bfloat16), new_weight, total))
        for p in range(pairs):
            weights, new_weight, total = weighed[p]
            mixed = sum(
                jnp.dot(
                    weights[:, at:at + positions // 2], values[p, at:at + positions // 2],
                    preferred_element_type=jnp.float32,
                )
                for at in (0, positions // 2)
            )
            mixed = jnp.where(first, mixed[:, :HEAD_SIZE], mixed[:, HEAD_SIZE:])
            o_s[p * 2 * hc:(p + 1) * 2 * hc, :] = (
                mixed + new_weight * pair_rows(value_new, p)
            ) / total
        for h in range(hc):
            cols = slice(starts[c] + h * HEAD_SIZE, starts[c] + (h + 1) * HEAD_SIZE)
            att_send[:, cols] = o_s[pl.ds(h, local_rows, stride=hc), :].astype(jnp.bfloat16)
        spread(c)

    partner = my + 1 - 2 * lax.rem(my, 2)
    far = lax.rem(my + 2, 4)
    far_leader = far + 1 - lax.rem(far, 2)

    leading = lax.rem(my, 2)

    def hand(o, slot, target):
        cols = pl.ds(*outs[o])
        return pltpu.make_async_remote_copy(
            src_ref=y_send.at[:, cols], dst_ref=y_recv.at[slot, :, cols],
            send_sem=ys_sem.at[lax.rem(slot, 2)], recv_sem=yr_sem.at[slot, o],
            device_id={"gy": target}, device_id_type=MESH,
        )

    def give(o):
        cols = pl.ds(*outs[o])
        return pltpu.make_async_remote_copy(
            src_ref=out.at[:, :, cols], dst_ref=out.at[:, :, cols],
            send_sem=os_sem, recv_sem=or_sem,
            device_id={"gy": partner}, device_id_type=MESH,
        )

    for c in range(last + 1):
        fs = slice(starts[c], starts[c] + widths[c])
        drain(att_recv.at[pl.ds(0, n - 1), :, pl.ds(starts[c], widths[c])], ar_sem.at[c])
        att_recv[me, :, fs] = att_send[:, fs]
        for j in range(n):
            block = att_recv[j, :, fs].astype(jnp.float32)
            for b in range(batches):
                x_s[b * rows + j * here:b * rows + (j + 1) * here, :widths[c]] = block[
                    b * here:(b + 1) * here, :
                ]
        xc = x_s[:, :widths[c]].astype(jnp.bfloat16)
        wo_copy(c).wait()
        for o in range(len(outs)):
            cols = slice(outs[o][0], outs[o][0] + outs[o][1])
            half = outs[o][1] // 2
            for at in (cols.start, cols.start + half):
                part = slice(at, at + half)
                y = jnp.dot(xc, wo[fs, part], preferred_element_type=jnp.float32)
                if c > 0:
                    y = y + ybuf[:, part]
                if c < last:
                    ybuf[:, part] = y
                else:
                    y_send[:, part] = y.astype(jnp.bfloat16)
            if c == last:
                hand(o, 1 - leading, far_leader).start()

    @pl.when(leader)
    def _():
        for o in range(len(outs)):
            cols = slice(outs[o][0], outs[o][0] + outs[o][1])
            for slot in (0, 2, 1):
                hand(o, slot, far).wait_recv()
            parts = [y_recv[slot, :, cols].astype(jnp.float32) for slot in range(3)]
            y = (y_send[:, cols].astype(jnp.float32) + parts[0]) + (parts[1] + parts[2])
            y = y.reshape(batches, rows, outs[o][1])
            out[:, :, cols] = (tok[:, :, cols].astype(jnp.float32) + y).astype(jnp.bfloat16)
            give(o).start()
        drain(out, os_sem)

    @pl.when(follower)
    def _():
        for o in range(len(outs)):
            hand(o, 2, partner).start()
        drain(y_send, ys_sem.at[0])
        drain(out, or_sem)

    drain(y_send, ys_sem.at[1 - leading])
    drain(send.at[pl.ds(0, n - 1)], qs_sem)
    drain(att_recv.at[pl.ds(0, n - 1)], as_sem)


def local(n, ny, tokens, lengths, norm_gain, w_query, key_value_weight, w_out, cache):
    batches, rows, depth = tokens.shape
    here = rows // n
    local_rows = batches * here
    q_width = w_query.shape[1]
    kv_heads = key_value_weight.shape[1]
    kv_width = kv_heads * key_value_weight.shape[2]
    assert kv_heads == 1 and ny == 4 and local_rows % 2 == 0
    heads = q_width // HEAD_SIZE
    out_width = w_out.shape[1]
    quarter = heads // 4
    chunks = (quarter,) * 4
    phases = (2 * quarter, quarter, quarter)
    splits = tuple(max(1, depth * p * HEAD_SIZE // (1 << 20)) for p in chunks)
    ahead = 4
    step = max(out_width // 8, 2 * HEAD_SIZE)
    outs = [(0, step)]
    while outs[-1][0] + outs[-1][1] < out_width:
        start = sum(outs[-1])
        outs.append((start, step if start < 2 * step else 2 * step))
    freq = np.float32(ROPE_BASE) ** (
        -2.0 * np.arange(HEAD_SIZE // 2, dtype=np.float32) / HEAD_SIZE
    )
    freq = np.concatenate([freq, freq]).astype(np.float32)[None, :]
    positions = cache.shape[2]
    interleaved = cache.reshape(local_rows * positions * 2, HEAD_SIZE)
    hbm = pl.BlockSpec(memory_space=pltpu.HBM)
    f32, bf16 = jnp.float32, jnp.bfloat16
    dma = pltpu.SemaphoreType.DMA
    total_rows = batches * rows
    wide = q_width + kv_width + HEAD_SIZE
    most = max(phases)
    return pl.pallas_call(
        functools.partial(kernel, n, ny, chunks, splits, phases, ahead, outs),
        out_shape=pltpu.VMEM(tokens.shape, bf16),
        in_specs=[hbm] * 8,
        out_specs=pl.BlockSpec(memory_space=pltpu.VMEM),
        scratch_shapes=[
            pltpu.SMEM(lengths.shape, jnp.int32),
            pltpu.VMEM(tokens.shape, bf16),
            pltpu.VMEM((depth // HEAD_SIZE, HEAD_SIZE), bf16),
            pltpu.VMEM((1, HEAD_SIZE), f32),
            pltpu.VMEM(w_query.shape, bf16),
            pltpu.VMEM((depth, kv_width), bf16),
            pltpu.VMEM(w_out.shape, bf16),
            pltpu.VMEM(interleaved.shape, bf16),
            pltpu.VMEM((total_rows, depth), bf16),
            pltpu.VMEM((total_rows, most * HEAD_SIZE), f32),
            pltpu.VMEM((positions, HEAD_SIZE), f32),
            pltpu.VMEM((local_rows // 2, positions, 2 * HEAD_SIZE), bf16),
            pltpu.VMEM((local_rows // 2, positions, 2 * HEAD_SIZE), bf16),
            pltpu.VMEM((n, local_rows, wide), f32),
            pltpu.VMEM((n, local_rows, wide), f32),
            pltpu.VMEM((local_rows * most, HEAD_SIZE), f32),
            pltpu.VMEM((local_rows * most, HEAD_SIZE), f32),
            pltpu.VMEM((local_rows, q_width), bf16),
            pltpu.VMEM((n, local_rows, q_width), bf16),
            pltpu.VMEM((total_rows, most * HEAD_SIZE), f32),
            pltpu.VMEM((total_rows, out_width), f32),
            pltpu.VMEM((total_rows, out_width), bf16),
            pltpu.VMEM((3, total_rows, out_width), bf16),
            dma((4,)), dma((ahead,)), dma((len(phases),)), dma,
            dma, dma((len(chunks) + 1,)), dma, dma((len(phases),)),
            dma((2,)), dma((3, len(outs))), dma, dma,
        ],
        compiler_params=pltpu.CompilerParams(
            collective_id=0, has_side_effects=True, vmem_limit_bytes=67043328 - 2 * tokens.size
        ),
    )(
        lengths, tokens, norm_gain.reshape(depth // HEAD_SIZE, HEAD_SIZE), jnp.asarray(freq),
        w_query, key_value_weight.reshape(depth, kv_width), w_out, interleaved,
    )


def solution(mesh):
    placed = (
        P(None, "groups", "gx"),
        P(None, ("groups", "gx")),
        P("gx"),
        P("gx", "gy"),
        P("gx", "gy", None),
        P("gy", "gx"),
        P(None, ("groups", "gx"), None, "gy", None, None),
    )
    return jax.shard_map(
        functools.partial(local, mesh.shape["gx"], mesh.shape["gy"]),
        mesh=mesh, in_specs=placed, out_specs=P(None, "groups", "gx"), check_vma=False,
    )
```

```python
import functools

import jax
import jax.numpy as jnp
import numpy as np
from jax import lax
from jax.experimental import pallas as pl
from jax.experimental.pallas import tpu as pltpu
from jax.sharding import PartitionSpec as P

MODEL_WIDTH = 16384
HEAD_SIZE = 128
ROPE_BASE = 500000.0
MESH = pl.DeviceIdType.MESH


def kernel(
    n, ny, chunks, splits, phases, ahead, outs,
    lens_hbm, tok_hbm, gain_hbm, freq_hbm, wq_hbm, wk_hbm, wo_hbm, kv_hbm,
    out,
    lens, tok, gain, freq, wq, wk, wo, kv, normed,
    acc, wide_s, keys, values, send, recv, q_s, o_s, att_send, att_recv, x_s,
    ybuf, y_send, y_recv,
    small_sem, stream_sem, qs_sem, qr_sem, as_sem, ar_sem, ys_sem, yr_sem, out_sem,
):
    batches, rows, depth = tok.shape
    here = rows // n
    total_rows = batches * rows
    q_width = wq.shape[1]
    kv_width = wk.shape[1]
    out_width = wo.shape[1]
    local_rows = batches * here
    pairs = local_rows // 2
    positions = keys.shape[1]
    last = len(phases) - 1
    starts = [sum(phases[:i]) * HEAD_SIZE for i in range(len(phases))]
    widths = [heads * HEAD_SIZE for heads in phases]
    nc = len(chunks)
    q_starts = [sum(chunks[:i]) * HEAD_SIZE for i in range(nc)]
    q_widths = [heads * HEAD_SIZE for heads in chunks]
    me = lax.axis_index("gx")
    my = lax.axis_index("gy")
    leader = lax.rem(my, 2) == 1
    follower = lax.rem(my, 2) == 0

    small = [
        pltpu.make_async_copy(tok_hbm, tok, small_sem.at[0]),
        pltpu.make_async_copy(gain_hbm, gain, small_sem.at[1]),
        pltpu.make_async_copy(freq_hbm, freq, small_sem.at[2]),
        pltpu.make_async_copy(lens_hbm, lens, small_sem.at[3]),
    ]

    pieces = [(wk_hbm, wk)]
    for c in range(nc):
        for begin, end in splits[c]:
            at = (pl.ds(begin, end - begin), pl.ds(q_starts[c], q_widths[c]))
            pieces.append((wq_hbm.at[at], wq.at[at]))

    for r in range(local_rows):
        at = pl.ds(r * 2 * positions, 2 * positions)
        pieces.append((kv_hbm.at[at], kv.at[at]))

    def stream(i):
        return pltpu.make_async_copy(*pieces[i], stream_sem.at[i % ahead])

    def take(i):
        stream(i).wait()
        if i + ahead < len(pieces):
            stream(i + ahead).start()

    def wo_copy(c):
        at = pl.ds(starts[c], widths[c])
        return pltpu.make_async_copy(wo_hbm.at[at], wo.at[at], stream_sem.at[c])

    for copy in small:
        copy.start()
    for i in range(ahead):
        stream(i).start()

    barrier = pltpu.get_barrier_semaphore()

    def each(fn):
        if n <= 8:
            for d in range(1, n):
                fn(d)
        else:
            def body(d, carry):
                fn(d)
                return carry
            lax.fori_loop(1, n, body, 0)

    def greet(d):
        pl.semaphore_signal(
            barrier, inc=1, device_id={"gx": lax.rem(me + d, n)}, device_id_type=MESH
        )

    each(greet)

    for d in range(1, ny):
        pl.semaphore_signal(
            barrier, inc=1, device_id={"gy": lax.rem(my + d, ny)}, device_id_type=MESH
        )

    def to(d):
        return lax.rem(me + d, n)

    def drain(ref, sem):
        pltpu.make_async_copy(ref, ref, sem).wait()

    small[0].wait()
    small[1].wait()
    x = tok[...].astype(jnp.float32).reshape(total_rows, depth)
    for k in range(depth // HEAD_SIZE):
        cols = slice(k * HEAD_SIZE, (k + 1) * HEAD_SIZE)
        normed[:, cols] = (x[:, cols] * gain[k:k + 1, :].astype(jnp.float32)).astype(jnp.bfloat16)
    squares = jnp.broadcast_to(jnp.sum(x * x, axis=1, keepdims=True), (total_rows, HEAD_SIZE))

    def put(part, start):
        width = part.shape[1]
        for j in range(n):
            for b in range(batches):
                send[j, b * here:(b + 1) * here, start:start + width] = part[
                    b * rows + j * here:b * rows + (j + 1) * here, :
                ]

    def put_halves(start, width):
        for j in range(n):
            for b in range(batches):
                at = slice(b * rows + j * here, b * rows + (j + 1) * here)
                send[j, b * here:(b + 1) * here, start:start + width] = (
                    acc[at, :width] + acc[at, width:2 * width]
                )

    def shift(c, start, width):
        cols = pl.ds(start, width)
        def one(d):
            pltpu.make_async_remote_copy(
                src_ref=send.at[to(d), :, cols], dst_ref=recv.at[me, :, cols],
                send_sem=qs_sem, recv_sem=qr_sem.at[c],
                device_id={"gx": to(d)}, device_id_type=MESH,
            ).start()
        each(one)

    def arrived(c, start, width):
        drain(recv.at[pl.ds(0, n - 1), :, pl.ds(start, width)], qr_sem.at[c])

    def summed(start, width):
        cols = pl.ds(start, width)
        def add(d, acc):
            return acc + recv[to(d), :, cols]
        return lax.fori_loop(1, n, add, send[me, :, cols], unroll=n <= 8)

    side = kv_width + HEAD_SIZE
    take(0)
    middle = depth // 2
    for k in range(2):
        ks = slice(k * middle, (k + 1) * middle)
        acc[:, k * kv_width:(k + 1) * kv_width] = jnp.dot(
            normed[:, ks], wk[ks], preferred_element_type=jnp.float32
        )
    put_halves(q_width, kv_width)
    put(squares, q_width + kv_width)
    i = 1
    for c in range(nc):
        for k, (begin, end) in enumerate(splits[c]):
            take(i)
            i += 1
            narrow = q_widths[c] == 2 * HEAD_SIZE
            half = q_widths[c] if narrow else q_widths[c] // 2
            size = (end - begin) // 2 if narrow else end - begin
            for m in range(2):
                at = 0 if narrow else m * half
                ks = slice(begin + m * size, begin + (m + 1) * size) if narrow else slice(begin, end)
                piece = jnp.dot(
                    normed[:, ks], wq[ks, q_starts[c] + at:q_starts[c] + at + half],
                    preferred_element_type=jnp.float32,
                )
                into = slice(m * half, (m + 1) * half)
                if k > 0:
                    piece = piece + acc[:, into]
                if narrow or k < len(splits[c]) - 1:
                    acc[:, into] = piece
                else:
                    put(piece, q_starts[c] + at)
        if narrow:
            put_halves(q_starts[c], half)
        if c == 0:
            pl.semaphore_wait(barrier, n - 1 + ny - 1)
            shift(nc, q_width, side)
        shift(c, q_starts[c], q_widths[c])

    small[2].wait()
    small[3].wait()
    lane = lax.broadcasted_iota(jnp.int32, (local_rows, HEAD_SIZE), 1)
    row = lax.broadcasted_iota(jnp.int32, (local_rows, HEAD_SIZE), 0)
    place = jnp.zeros((local_rows, HEAD_SIZE), jnp.float32)
    for r in range(local_rows):
        place = jnp.where(row == r, lens[r // here, r % here].astype(jnp.float32), place)
    angle = place * freq[...]
    cosine = jnp.cos(angle)
    sine = jnp.sin(angle)
    sine = jnp.where(lane < HEAD_SIZE // 2, -sine, sine)

    def rotate(v):
        return v * cosine + pltpu.roll(v, HEAD_SIZE // 2, 1) * sine

    block_rows = wide_s.shape[0]
    blocks = 2 * positions // block_rows

    def divide(t, carry):
        r = t // blocks
        wide_s[...] = kv[pl.ds(pl.multiple_of(t * block_rows, block_rows), block_rows), :].astype(
            jnp.float32
        )
        half = block_rows // 2
        at = pl.ds(pl.multiple_of(lax.rem(t, blocks) * half, half), half)
        lanes = pl.ds(pl.multiple_of(lax.rem(r, 2) * HEAD_SIZE, HEAD_SIZE), HEAD_SIZE)
        keys[r // 2, at, lanes] = wide_s[pl.ds(0, half, stride=2), :].astype(jnp.bfloat16)
        values[r // 2, at, lanes] = wide_s[pl.ds(1, half, stride=2), :].astype(jnp.bfloat16)
        return carry

    for r in range(local_rows):
        take(i)
        i += 1
        lax.fori_loop(r * blocks, (r + 1) * blocks, divide, 0)
    for c in range(last + 1):
        wo_copy(c).start()

    arrived(nc, q_width, side)
    tail = summed(q_width, side)
    scale = lax.rsqrt(tail[:, kv_width:] / MODEL_WIDTH + 1e-05)
    rkey = rotate(tail[:, :HEAD_SIZE] * scale)
    value_new = tail[:, HEAD_SIZE:2 * HEAD_SIZE] * scale
    inv_root = np.float32(1.0 / np.sqrt(np.float32(HEAD_SIZE)))

    def spread(c):
        cols = pl.ds(starts[c], widths[c])
        def one(d):
            pltpu.make_async_remote_copy(
                src_ref=att_send.at[:, cols], dst_ref=att_recv.at[me, :, cols],
                send_sem=as_sem, recv_sem=ar_sem.at[c],
                device_id={"gx": to(d)}, device_id_type=MESH,
            ).start()
        each(one)

    for c in range(last + 1):
        hc = phases[c]
        for k in range(nc):
            if starts[c] <= q_starts[k] < starts[c] + widths[c]:
                arrived(k, q_starts[k], q_widths[k])
        block = summed(starts[c], widths[c])
        for h in range(hc):
            q_s[pl.ds(h, local_rows, stride=hc), :] = rotate(
                block[:, h * HEAD_SIZE:(h + 1) * HEAD_SIZE] * scale
            )
        column = lax.broadcasted_iota(jnp.int32, (2 * hc, positions), 1)
        first = lax.broadcasted_iota(jnp.int32, (2 * hc, HEAD_SIZE), 0) < hc
        first_wide = lax.broadcasted_iota(jnp.int32, (2 * hc, positions), 0) < hc

        def pair_rows(v, p):
            shape = (2 * hc, v.shape[1])
            return jnp.where(
                first,
                jnp.broadcast_to(v[2 * p:2 * p + 1], shape),
                jnp.broadcast_to(v[2 * p + 1:2 * p + 2], shape),
            )

        weighed = []
        for p in range(pairs):
            query = q_s[p * 2 * hc:(p + 1) * 2 * hc, :].astype(jnp.bfloat16).astype(jnp.float32)
            both = jnp.concatenate(
                [jnp.where(first, query, 0.0), jnp.where(first, 0.0, query)], axis=1
            ).astype(jnp.bfloat16)
            scores = jnp.concatenate(
                [
                    lax.dot_general(
                        both, keys[p, at:at + positions // 2], (((1,), (1,)), ((), ())),
                        preferred_element_type=jnp.float32,
                    )
                    for at in (0, positions // 2)
                ],
                axis=1,
            ) * inv_root
            r = 2 * p
            limit = jnp.where(
                first_wide, lens[r // here, r % here], lens[(r + 1) // here, (r + 1) % here]
            )
            scores = jnp.where(column < limit, scores, -1e30)
            new_score = jnp.sum(query * pair_rows(rkey, p), axis=1, keepdims=True) * inv_root
            top = jnp.maximum(jnp.max(scores, axis=1, keepdims=True), new_score)
            weights = jnp.exp(scores - top)
            new_weight = jnp.exp(new_score - top)
            total = jnp.sum(weights, axis=1, keepdims=True) + new_weight
            weighed.append((weights.astype(jnp.bfloat16), new_weight, total))
        for p in range(pairs):
            weights, new_weight, total = weighed[p]
            mixed = sum(
                jnp.dot(
                    weights[:, at:at + positions // 2], values[p, at:at + positions // 2],
                    preferred_element_type=jnp.float32,
                )
                for at in (0, positions // 2)
            )
            mixed = jnp.where(first, mixed[:, :HEAD_SIZE], mixed[:, HEAD_SIZE:])
            o_s[p * 2 * hc:(p + 1) * 2 * hc, :] = (
                mixed + new_weight * pair_rows(value_new, p)
            ) / total
        for h in range(hc):
            cols = slice(starts[c] + h * HEAD_SIZE, starts[c] + (h + 1) * HEAD_SIZE)
            att_send[:, cols] = o_s[pl.ds(h, local_rows, stride=hc), :].astype(jnp.bfloat16)
        spread(c)

    partner = my + 1 - 2 * lax.rem(my, 2)
    far = lax.rem(my + 2, 4)
    far_leader = far + 1 - lax.rem(far, 2)

    def hand(o, slot, target):
        cols = pl.ds(*outs[o])
        return pltpu.make_async_remote_copy(
            src_ref=y_send.at[:, cols], dst_ref=y_recv.at[slot, :, cols],
            send_sem=ys_sem, recv_sem=yr_sem.at[o],
            device_id={"gy": target}, device_id_type=MESH,
        )

    def give(o):
        cols = pl.ds(*outs[o])
        return pltpu.make_async_remote_copy(
            src_ref=out.at[:, :, cols], dst_ref=out.at[:, :, cols],
            send_sem=out_sem, recv_sem=out_sem,
            device_id={"gy": partner}, device_id_type=MESH,
        )

    def product(o, fs, xc):
        start, width = outs[o]
        for at in (start, start + width // 2):
            part = slice(at, at + width // 2)
            yield part, jnp.dot(xc, wo[fs, part], preferred_element_type=jnp.float32)

    for c in range(last + 1):
        fs = slice(starts[c], starts[c] + widths[c])
        drain(att_recv.at[pl.ds(0, n - 1), :, pl.ds(starts[c], widths[c])], ar_sem.at[c])
        att_recv[me, :, fs] = att_send[:, fs]
        for j in range(n):
            block = att_recv[j, :, fs].astype(jnp.float32)
            for b in range(batches):
                x_s[b * rows + j * here:b * rows + (j + 1) * here, :widths[c]] = block[
                    b * here:(b + 1) * here, :
                ]
        xc = x_s[:, :widths[c]].astype(jnp.bfloat16)
        wo_copy(c).wait()
        if c < last:
            for o in range(len(outs)):
                for part, y in product(o, fs, xc):
                    ybuf[:, part] = y + ybuf[:, part] if c > 0 else y

    for o in range(len(outs)):
        for part, y in product(o, fs, xc):
            y_send[:, part] = (y + ybuf[:, part]).astype(jnp.bfloat16)
        hand(o, 1 - lax.rem(my, 2), far_leader).start()

    @pl.when(leader)
    def _():
        for o in range(len(outs)):
            cols = slice(outs[o][0], outs[o][0] + outs[o][1])
            drain(y_recv.at[:, :, cols], yr_sem.at[o])
            parts = [y_recv[slot, :, cols].astype(jnp.float32) for slot in range(3)]
            y = (y_send[:, cols].astype(jnp.float32) + parts[0]) + (parts[1] + parts[2])
            y = y.reshape(batches, rows, outs[o][1])
            out[:, :, cols] = (tok[:, :, cols].astype(jnp.float32) + y).astype(jnp.bfloat16)
            give(o).start()
        drain(y_send, ys_sem)

    @pl.when(follower)
    def _():
        for o in range(len(outs)):
            hand(o, 2, partner).start()
        drain(y_recv.at[0:2], ys_sem)

    drain(out, out_sem)
    drain(send.at[pl.ds(0, n - 1)], qs_sem)
    drain(att_recv.at[pl.ds(0, n - 1)], as_sem)


def local(n, ny, tokens, lengths, norm_gain, w_query, key_value_weight, w_out, cache):
    batches, rows, depth = tokens.shape
    here = rows // n
    local_rows = batches * here
    q_width = w_query.shape[1]
    kv_heads = key_value_weight.shape[1]
    kv_width = kv_heads * key_value_weight.shape[2]
    assert kv_heads == 1 and ny == 4 and local_rows % 2 == 0
    heads = q_width // HEAD_SIZE
    out_width = w_out.shape[1]
    quarter = heads // 4
    chunks = (quarter,) * 3 + (quarter // 2,) * 2
    phases = (2 * quarter, 2 * quarter)
    cuts = []
    for c, width in enumerate(chunks):
        parts = max(1, depth * width * HEAD_SIZE >> 20)
        size = depth // parts
        cut = [(k * size, (k + 1) * size) for k in range(parts)]
        if c == len(chunks) - 1 and size % 512 == 0:
            begin, end = cut.pop()
            middle = (begin + end) // 2
            cut += [(begin, middle), (middle, end)]
        cuts.append(cut)
    ahead = 4
    step = min(1024, out_width)
    outs = [(start, step) for start in range(0, out_width, step)]
    freq = np.float32(ROPE_BASE) ** (
        -2.0 * np.arange(HEAD_SIZE // 2, dtype=np.float32) / HEAD_SIZE
    )
    freq = np.concatenate([freq, freq]).astype(np.float32)[None, :]
    positions = cache.shape[2]
    interleaved = cache.reshape(local_rows * positions * 2, HEAD_SIZE)
    hbm = pl.BlockSpec(memory_space=pltpu.HBM)
    f32, bf16 = jnp.float32, jnp.bfloat16
    dma = pltpu.SemaphoreType.DMA
    total_rows = batches * rows
    wide = q_width + kv_width + HEAD_SIZE
    most = max(phases)
    return pl.pallas_call(
        functools.partial(kernel, n, ny, chunks, cuts, phases, ahead, outs),
        out_shape=pltpu.VMEM(tokens.shape, bf16),
        in_specs=[hbm] * 8,
        out_specs=pl.BlockSpec(memory_space=pltpu.VMEM),
        scratch_shapes=[
            pltpu.SMEM(lengths.shape, jnp.int32),
            pltpu.VMEM(tokens.shape, bf16),
            pltpu.VMEM((depth // HEAD_SIZE, HEAD_SIZE), bf16),
            pltpu.VMEM((1, HEAD_SIZE), f32),
            pltpu.VMEM(w_query.shape, bf16),
            pltpu.VMEM((depth, kv_width), bf16),
            pltpu.VMEM(w_out.shape, bf16),
            pltpu.VMEM(interleaved.shape, bf16),
            pltpu.VMEM((total_rows, depth), bf16),
            pltpu.VMEM((total_rows, most * HEAD_SIZE), f32),
            pltpu.VMEM((positions, HEAD_SIZE), f32),
            pltpu.VMEM((local_rows // 2, positions, 2 * HEAD_SIZE), bf16),
            pltpu.VMEM((local_rows // 2, positions, 2 * HEAD_SIZE), bf16),
            pltpu.VMEM((n, local_rows, wide), f32),
            pltpu.VMEM((n, local_rows, wide), f32),
            pltpu.VMEM((local_rows * most, HEAD_SIZE), f32),
            pltpu.VMEM((local_rows * most, HEAD_SIZE), f32),
            pltpu.VMEM((local_rows, q_width), bf16),
            pltpu.VMEM((n, local_rows, q_width), bf16),
            pltpu.VMEM((total_rows, most * HEAD_SIZE), f32),
            pltpu.VMEM((total_rows, out_width), f32),
            pltpu.VMEM((total_rows, out_width), bf16),
            pltpu.VMEM((3, total_rows, out_width), bf16),
            dma((4,)), dma((ahead,)), dma, dma((len(chunks) + 1,)),
            dma, dma((len(phases),)), dma, dma((len(outs),)), dma,
        ],
        compiler_params=pltpu.CompilerParams(
            collective_id=0, has_side_effects=True, vmem_limit_bytes=67043328 - 2 * tokens.size
        ),
    )(
        lengths, tokens, norm_gain.reshape(depth // HEAD_SIZE, HEAD_SIZE), jnp.asarray(freq),
        w_query, key_value_weight.reshape(depth, kv_width), w_out, interleaved,
    )


def solution(mesh):
    placed = (
        P(None, "groups", "gx"),
        P(None, ("groups", "gx")),
        P("gx"),
        P("gx", "gy"),
        P("gx", "gy", None),
        P("gy", "gx"),
        P(None, ("groups", "gx"), None, "gy", None, None),
    )
    return jax.shard_map(
        functools.partial(local, mesh.shape["gx"], mesh.shape["gy"]),
        mesh=mesh, in_specs=placed, out_specs=P(None, "groups", "gx"), check_vma=False,
    )
```

```python
import functools

import jax
import jax.numpy as jnp
import numpy as np
from jax import lax
from jax.experimental import pallas as pl
from jax.experimental.pallas import tpu as pltpu
from jax.sharding import PartitionSpec as P

MODEL_WIDTH = 16384
HEAD_SIZE = 128
ROPE_BASE = 500000.0
MESH = pl.DeviceIdType.MESH


def kernel(
    n, ny, chunks, splits, phases, ahead, outs,
    lens_hbm, tok_hbm, gain_hbm, freq_hbm, wq_hbm, wk_hbm, wo_hbm, kv_hbm,
    out,
    lens, tok, gain, freq, wq, wk, wo, kv, normed,
    acc, wide_s, keys, values, send, recv, q_s, o_s, att_send, att_recv, x_s,
    ybuf, y_send, y_recv,
    small_sem, stream_sem, qs_sem, qr_sem, as_sem, ar_sem, ys_sem, yr_sem, out_sem,
):
    batches, rows, depth = tok.shape
    here = rows // n
    total_rows = batches * rows
    q_width = wq.shape[1]
    kv_width = wk.shape[1]
    out_width = wo.shape[1]
    local_rows = batches * here
    pairs = local_rows // 2
    positions = keys.shape[1]
    last = len(phases) - 1
    starts = [sum(phases[:i]) * HEAD_SIZE for i in range(len(phases))]
    widths = [heads * HEAD_SIZE for heads in phases]
    nc = len(chunks)
    q_starts = [sum(chunks[:i]) * HEAD_SIZE for i in range(nc)]
    q_widths = [heads * HEAD_SIZE for heads in chunks]
    me = lax.axis_index("gx")
    my = lax.axis_index("gy")
    leader = lax.rem(my, 2) == 1
    follower = lax.rem(my, 2) == 0

    small = [
        pltpu.make_async_copy(tok_hbm, tok, small_sem.at[0]),
        pltpu.make_async_copy(gain_hbm, gain, small_sem.at[1]),
        pltpu.make_async_copy(freq_hbm, freq, small_sem.at[2]),
        pltpu.make_async_copy(lens_hbm, lens, small_sem.at[3]),
    ]

    pieces = [(wk_hbm, wk)]
    for c in range(nc):
        for begin, end in splits[c]:
            at = (pl.ds(begin, end - begin), pl.ds(q_starts[c], q_widths[c]))
            pieces.append((wq_hbm.at[at], wq.at[at]))

    for r in range(local_rows):
        at = pl.ds(r * 2 * positions, 2 * positions)
        pieces.append((kv_hbm.at[at], kv.at[at]))

    def stream(i):
        return pltpu.make_async_copy(*pieces[i], stream_sem.at[i % ahead])

    def take(i):
        stream(i).wait()
        if i + ahead < len(pieces):
            stream(i + ahead).start()

    def wo_copy(c):
        at = pl.ds(starts[c], widths[c])
        return pltpu.make_async_copy(wo_hbm.at[at], wo.at[at], stream_sem.at[c])

    for copy in small:
        copy.start()
    for i in range(ahead):
        stream(i).start()

    barrier = pltpu.get_barrier_semaphore()

    def each(fn):
        if n <= 8:
            for d in range(1, n):
                fn(d)
        else:
            def body(d, carry):
                fn(d)
                return carry
            lax.fori_loop(1, n, body, 0)

    def greet(d):
        pl.semaphore_signal(
            barrier, inc=1, device_id={"gx": lax.rem(me + d, n)}, device_id_type=MESH
        )

    each(greet)

    for d in range(1, ny):
        pl.semaphore_signal(
            barrier, inc=1, device_id={"gy": lax.rem(my + d, ny)}, device_id_type=MESH
        )

    def to(d):
        return lax.rem(me + d, n)

    def drain(ref, sem):
        pltpu.make_async_copy(ref, ref, sem).wait()

    small[0].wait()
    small[1].wait()
    x = tok[...].astype(jnp.float32).reshape(total_rows, depth)
    for k in range(depth // HEAD_SIZE):
        cols = slice(k * HEAD_SIZE, (k + 1) * HEAD_SIZE)
        normed[:, cols] = (x[:, cols] * gain[k:k + 1, :].astype(jnp.float32)).astype(jnp.bfloat16)
    squares = jnp.broadcast_to(jnp.sum(x * x, axis=1, keepdims=True), (total_rows, HEAD_SIZE))

    def put(part, start):
        width = part.shape[1]
        for j in range(n):
            for b in range(batches):
                send[j, b * here:(b + 1) * here, start:start + width] = part[
                    b * rows + j * here:b * rows + (j + 1) * here, :
                ]

    def put_halves(start, width):
        for j in range(n):
            for b in range(batches):
                at = slice(b * rows + j * here, b * rows + (j + 1) * here)
                send[j, b * here:(b + 1) * here, start:start + width] = (
                    acc[at, :width] + acc[at, width:2 * width]
                )

    def shift(c, start, width):
        cols = pl.ds(start, width)
        def one(d):
            pltpu.make_async_remote_copy(
                src_ref=send.at[to(d), :, cols], dst_ref=recv.at[me, :, cols],
                send_sem=qs_sem, recv_sem=qr_sem.at[c],
                device_id={"gx": to(d)}, device_id_type=MESH,
            ).start()
        each(one)

    def arrived(c, start, width):
        drain(recv.at[pl.ds(0, n - 1), :, pl.ds(start, width)], qr_sem.at[c])

    def summed(start, width):
        cols = pl.ds(start, width)
        def add(d, acc):
            return acc + recv[to(d), :, cols]
        return lax.fori_loop(1, n, add, send[me, :, cols], unroll=n <= 8)

    side = kv_width + HEAD_SIZE
    take(0)
    middle = depth // 2
    for k in range(2):
        ks = slice(k * middle, (k + 1) * middle)
        acc[:, k * kv_width:(k + 1) * kv_width] = jnp.dot(
            normed[:, ks], wk[ks], preferred_element_type=jnp.float32
        )
    put_halves(q_width, kv_width)
    put(squares, q_width + kv_width)
    i = 1
    for c in range(nc):
        for k, (begin, end) in enumerate(splits[c]):
            take(i)
            i += 1
            narrow = q_widths[c] == 2 * HEAD_SIZE
            half = q_widths[c] if narrow else q_widths[c] // 2
            size = (end - begin) // 2 if narrow else end - begin
            for m in range(2):
                at = 0 if narrow else m * half
                ks = slice(begin + m * size, begin + (m + 1) * size) if narrow else slice(begin, end)
                piece = jnp.dot(
                    normed[:, ks], wq[ks, q_starts[c] + at:q_starts[c] + at + half],
                    preferred_element_type=jnp.float32,
                )
                into = slice(m * half, (m + 1) * half)
                if k > 0:
                    piece = piece + acc[:, into]
                if narrow or k < len(splits[c]) - 1:
                    acc[:, into] = piece
                else:
                    put(piece, q_starts[c] + at)
        if narrow:
            put_halves(q_starts[c], half)
        if c == 0:
            pl.semaphore_wait(barrier, n - 1 + ny - 1)
            shift(nc, q_width, side)
        shift(c, q_starts[c], q_widths[c])

    small[2].wait()
    small[3].wait()
    lane = lax.broadcasted_iota(jnp.int32, (local_rows, HEAD_SIZE), 1)
    row = lax.broadcasted_iota(jnp.int32, (local_rows, HEAD_SIZE), 0)
    place = jnp.zeros((local_rows, HEAD_SIZE), jnp.float32)
    for r in range(local_rows):
        place = jnp.where(row == r, lens[r // here, r % here].astype(jnp.float32), place)
    angle = place * freq[...]
    cosine = jnp.cos(angle)
    sine = jnp.sin(angle)
    sine = jnp.where(lane < HEAD_SIZE // 2, -sine, sine)

    def rotate(v):
        return v * cosine + pltpu.roll(v, HEAD_SIZE // 2, 1) * sine

    block_rows = wide_s.shape[0]
    blocks = 2 * positions // block_rows

    def divide(t, carry):
        r = t // blocks
        wide_s[...] = kv[pl.ds(pl.multiple_of(t * block_rows, block_rows), block_rows), :].astype(
            jnp.float32
        )
        half = block_rows // 2
        at = pl.ds(pl.multiple_of(lax.rem(t, blocks) * half, half), half)
        lanes = pl.ds(pl.multiple_of(lax.rem(r, 2) * HEAD_SIZE, HEAD_SIZE), HEAD_SIZE)
        keys[r // 2, at, lanes] = wide_s[pl.ds(0, half, stride=2), :].astype(jnp.bfloat16)
        values[r // 2, at, lanes] = wide_s[pl.ds(1, half, stride=2), :].astype(jnp.bfloat16)
        return carry

    for r in range(local_rows):
        take(i)
        i += 1
        lax.fori_loop(r * blocks, (r + 1) * blocks, divide, 0)
    for c in range(last + 1):
        wo_copy(c).start()

    arrived(nc, q_width, side)
    tail = summed(q_width, side)
    scale = lax.rsqrt(tail[:, kv_width:] / MODEL_WIDTH + 1e-05)
    rkey = rotate(tail[:, :HEAD_SIZE] * scale)
    value_new = tail[:, HEAD_SIZE:2 * HEAD_SIZE] * scale
    inv_root = np.float32(1.0 / np.sqrt(np.float32(HEAD_SIZE)))

    def spread(c):
        cols = pl.ds(starts[c], widths[c])
        def one(d):
            pltpu.make_async_remote_copy(
                src_ref=att_send.at[:, cols], dst_ref=att_recv.at[me, :, cols],
                send_sem=as_sem, recv_sem=ar_sem.at[c],
                device_id={"gx": to(d)}, device_id_type=MESH,
            ).start()
        each(one)

    for c in range(last + 1):
        hc = phases[c]
        for k in range(nc):
            if starts[c] <= q_starts[k] < starts[c] + widths[c]:
                arrived(k, q_starts[k], q_widths[k])
        block = summed(starts[c], widths[c])
        for h in range(hc):
            q_s[pl.ds(h, local_rows, stride=hc), :] = rotate(
                block[:, h * HEAD_SIZE:(h + 1) * HEAD_SIZE] * scale
            )
        column = lax.broadcasted_iota(jnp.int32, (2 * hc, positions), 1)
        first = lax.broadcasted_iota(jnp.int32, (2 * hc, HEAD_SIZE), 0) < hc
        first_wide = lax.broadcasted_iota(jnp.int32, (2 * hc, positions), 0) < hc

        def pair_rows(v, p):
            shape = (2 * hc, v.shape[1])
            return jnp.where(
                first,
                jnp.broadcast_to(v[2 * p:2 * p + 1], shape),
                jnp.broadcast_to(v[2 * p + 1:2 * p + 2], shape),
            )

        weighed = []
        for p in range(pairs):
            query = q_s[p * 2 * hc:(p + 1) * 2 * hc, :].astype(jnp.bfloat16).astype(jnp.float32)
            both = jnp.concatenate(
                [jnp.where(first, query, 0.0), jnp.where(first, 0.0, query)], axis=1
            ).astype(jnp.bfloat16)
            scores = jnp.concatenate(
                [
                    lax.dot_general(
                        both, keys[p, at:at + positions // 2], (((1,), (1,)), ((), ())),
                        preferred_element_type=jnp.float32,
                    )
                    for at in (0, positions // 2)
                ],
                axis=1,
            ) * inv_root
            r = 2 * p
            limit = jnp.where(
                first_wide, lens[r // here, r % here], lens[(r + 1) // here, (r + 1) % here]
            )
            scores = jnp.where(column < limit, scores, -1e30)
            new_score = jnp.sum(query * pair_rows(rkey, p), axis=1, keepdims=True) * inv_root
            top = jnp.maximum(jnp.max(scores, axis=1, keepdims=True), new_score)
            weights = jnp.exp(scores - top)
            new_weight = jnp.exp(new_score - top)
            total = jnp.sum(weights, axis=1, keepdims=True) + new_weight
            weighed.append((weights.astype(jnp.bfloat16), new_weight, total))
        for p in range(pairs):
            weights, new_weight, total = weighed[p]
            mixed = sum(
                jnp.dot(
                    weights[:, at:at + positions // 2], values[p, at:at + positions // 2],
                    preferred_element_type=jnp.float32,
                )
                for at in (0, positions // 2)
            )
            mixed = jnp.where(first, mixed[:, :HEAD_SIZE], mixed[:, HEAD_SIZE:])
            o_s[p * 2 * hc:(p + 1) * 2 * hc, :] = (
                mixed + new_weight * pair_rows(value_new, p)
            ) / total
        for h in range(hc):
            cols = slice(starts[c] + h * HEAD_SIZE, starts[c] + (h + 1) * HEAD_SIZE)
            att_send[:, cols] = o_s[pl.ds(h, local_rows, stride=hc), :].astype(jnp.bfloat16)
        spread(c)

    partner = my + 1 - 2 * lax.rem(my, 2)
    far = lax.rem(my + 2, 4)
    far_leader = far + 1 - lax.rem(far, 2)
    far_other = far + 1 - 2 * lax.rem(far, 2)
    final = len(outs) - 1
    final_cols = pl.ds(*outs[final])
    early_cols = pl.ds(0, outs[final][0])

    def hand(o, slot, target):
        cols = pl.ds(*outs[o])
        return pltpu.make_async_remote_copy(
            src_ref=y_send.at[:, cols], dst_ref=y_recv.at[slot, :, cols],
            send_sem=ys_sem.at[o // final if final else 1], recv_sem=yr_sem.at[o],
            device_id={"gy": target}, device_id_type=MESH,
        )

    def give(o):
        cols = pl.ds(*outs[o])
        return pltpu.make_async_remote_copy(
            src_ref=out.at[:, :, cols], dst_ref=out.at[:, :, cols],
            send_sem=out_sem, recv_sem=out_sem,
            device_id={"gy": partner}, device_id_type=MESH,
        )

    def product(o, fs, xc):
        start, width = outs[o]
        for at in (start, start + width // 2):
            part = slice(at, at + width // 2)
            yield part, jnp.dot(xc, wo[fs, part], preferred_element_type=jnp.float32)

    for c in range(last + 1):
        fs = slice(starts[c], starts[c] + widths[c])
        drain(att_recv.at[pl.ds(0, n - 1), :, pl.ds(starts[c], widths[c])], ar_sem.at[c])
        att_recv[me, :, fs] = att_send[:, fs]
        for j in range(n):
            block = att_recv[j, :, fs].astype(jnp.float32)
            for b in range(batches):
                x_s[b * rows + j * here:b * rows + (j + 1) * here, :widths[c]] = block[
                    b * here:(b + 1) * here, :
                ]
        xc = x_s[:, :widths[c]].astype(jnp.bfloat16)
        wo_copy(c).wait()
        if c < last:
            for o in range(len(outs)):
                for part, y in product(o, fs, xc):
                    ybuf[:, part] = y + ybuf[:, part] if c > 0 else y

    for o in range(len(outs)):
        for part, y in product(o, fs, xc):
            y_send[:, part] = (y + ybuf[:, part]).astype(jnp.bfloat16)
        if o < final:
            hand(o, 1 - lax.rem(my, 2), far_leader).start()
        else:
            hand(o, 0, far).start()
            hand(o, 1, far_other).start()
            hand(o, 2, partner).start()

    def total(o):
        cols = slice(outs[o][0], outs[o][0] + outs[o][1])
        drain(y_recv.at[:, :, cols], yr_sem.at[o])
        parts = [y_recv[slot, :, cols].astype(jnp.float32) for slot in range(3)]
        y = (y_send[:, cols].astype(jnp.float32) + parts[0]) + (parts[1] + parts[2])
        y = y.reshape(batches, rows, outs[o][1])
        out[:, :, cols] = (tok[:, :, cols].astype(jnp.float32) + y).astype(jnp.bfloat16)

    if final:
        @pl.when(leader)
        def _():
            for o in range(final):
                total(o)
                give(o).start()

        @pl.when(follower)
        def _():
            for o in range(final):
                hand(o, 2, partner).start()

    total(final)
    if final:
        @pl.when(leader)
        def _():
            drain(y_send.at[:, early_cols], ys_sem.at[0])

        @pl.when(follower)
        def _():
            drain(y_recv.at[0:2, :, early_cols], ys_sem.at[0])

        drain(out.at[:, :, early_cols], out_sem)
    drain(y_recv.at[:, :, final_cols], ys_sem.at[1])
    drain(send.at[pl.ds(0, n - 1)], qs_sem)
    drain(att_recv.at[pl.ds(0, n - 1)], as_sem)


def local(n, ny, tokens, lengths, norm_gain, w_query, key_value_weight, w_out, cache):
    batches, rows, depth = tokens.shape
    here = rows // n
    local_rows = batches * here
    q_width = w_query.shape[1]
    kv_heads = key_value_weight.shape[1]
    kv_width = kv_heads * key_value_weight.shape[2]
    assert kv_heads == 1 and ny == 4 and local_rows % 2 == 0
    heads = q_width // HEAD_SIZE
    out_width = w_out.shape[1]
    quarter = heads // 4
    chunks = (quarter,) * 3 + (quarter // 2,) * 2
    phases = (2 * quarter, 2 * quarter)
    cuts = []
    for c, width in enumerate(chunks):
        parts = max(1, depth * width * HEAD_SIZE >> 20)
        size = depth // parts
        cut = [(k * size, (k + 1) * size) for k in range(parts)]
        if c == len(chunks) - 1 and size % 512 == 0:
            begin, end = cut.pop()
            middle = (begin + end) // 2
            cut += [(begin, middle), (middle, end)]
        cuts.append(cut)
    ahead = 4
    step = min(1024, out_width)
    outs = [(start, step) for start in range(0, out_width, step)]
    freq = np.float32(ROPE_BASE) ** (
        -2.0 * np.arange(HEAD_SIZE // 2, dtype=np.float32) / HEAD_SIZE
    )
    freq = np.concatenate([freq, freq]).astype(np.float32)[None, :]
    positions = cache.shape[2]
    interleaved = cache.reshape(local_rows * positions * 2, HEAD_SIZE)
    hbm = pl.BlockSpec(memory_space=pltpu.HBM)
    f32, bf16 = jnp.float32, jnp.bfloat16
    dma = pltpu.SemaphoreType.DMA
    total_rows = batches * rows
    wide = q_width + kv_width + HEAD_SIZE
    most = max(phases)
    return pl.pallas_call(
        functools.partial(kernel, n, ny, chunks, cuts, phases, ahead, outs),
        out_shape=pltpu.VMEM(tokens.shape, bf16),
        in_specs=[hbm] * 8,
        out_specs=pl.BlockSpec(memory_space=pltpu.VMEM),
        scratch_shapes=[
            pltpu.SMEM(lengths.shape, jnp.int32),
            pltpu.VMEM(tokens.shape, bf16),
            pltpu.VMEM((depth // HEAD_SIZE, HEAD_SIZE), bf16),
            pltpu.VMEM((1, HEAD_SIZE), f32),
            pltpu.VMEM(w_query.shape, bf16),
            pltpu.VMEM((depth, kv_width), bf16),
            pltpu.VMEM(w_out.shape, bf16),
            pltpu.VMEM(interleaved.shape, bf16),
            pltpu.VMEM((total_rows, depth), bf16),
            pltpu.VMEM((total_rows, most * HEAD_SIZE), f32),
            pltpu.VMEM((positions, HEAD_SIZE), f32),
            pltpu.VMEM((local_rows // 2, positions, 2 * HEAD_SIZE), bf16),
            pltpu.VMEM((local_rows // 2, positions, 2 * HEAD_SIZE), bf16),
            pltpu.VMEM((n, local_rows, wide), f32),
            pltpu.VMEM((n, local_rows, wide), f32),
            pltpu.VMEM((local_rows * most, HEAD_SIZE), f32),
            pltpu.VMEM((local_rows * most, HEAD_SIZE), f32),
            pltpu.VMEM((local_rows, q_width), bf16),
            pltpu.VMEM((n, local_rows, q_width), bf16),
            pltpu.VMEM((total_rows, most * HEAD_SIZE), f32),
            pltpu.VMEM((total_rows, out_width), f32),
            pltpu.VMEM((total_rows, out_width), bf16),
            pltpu.VMEM((3, total_rows, out_width), bf16),
            dma((4,)), dma((ahead,)), dma, dma((len(chunks) + 1,)),
            dma, dma((len(phases),)), dma((2,)), dma((len(outs),)), dma,
        ],
        compiler_params=pltpu.CompilerParams(
            collective_id=0, has_side_effects=True, vmem_limit_bytes=67043328 - 2 * tokens.size
        ),
    )(
        lengths, tokens, norm_gain.reshape(depth // HEAD_SIZE, HEAD_SIZE), jnp.asarray(freq),
        w_query, key_value_weight.reshape(depth, kv_width), w_out, interleaved,
    )


def solution(mesh):
    placed = (
        P(None, "groups", "gx"),
        P(None, ("groups", "gx")),
        P("gx"),
        P("gx", "gy"),
        P("gx", "gy", None),
        P("gy", "gx"),
        P(None, ("groups", "gx"), None, "gy", None, None),
    )
    return jax.shard_map(
        functools.partial(local, mesh.shape["gx"], mesh.shape["gy"]),
        mesh=mesh, in_specs=placed, out_specs=P(None, "groups", "gx"), check_vma=False,
    )
```

```python
import functools

import jax
import jax.numpy as jnp
import numpy as np
from jax import lax
from jax.experimental import pallas as pl
from jax.experimental.pallas import tpu as pltpu
from jax.sharding import PartitionSpec as P

MODEL_WIDTH = 16384
HEAD_SIZE = 128
ROPE_BASE = 500000.0
MESH = pl.DeviceIdType.MESH


def kernel(
    n, ny, chunks, splits, phases, ahead, outs,
    lens_hbm, tok_hbm, gain_hbm, freq_hbm, wq_hbm, wk_hbm, wo_hbm, kv_hbm,
    out,
    lens, tok, gain, freq, wq, wk, wo, kv, normed,
    acc, wide_s, keys, values, send, recv, q_s, o_s, att_send, att_recv, x_s,
    ybuf, y_send, y_recv,
    small_sem, stream_sem, qs_sem, qr_sem, as_sem, ar_sem, ys_sem, yr_sem, out_sem,
):
    batches, rows, depth = tok.shape
    here = rows // n
    total_rows = batches * rows
    q_width = wq.shape[1]
    kv_width = wk.shape[1]
    out_width = wo.shape[1]
    local_rows = batches * here
    pairs = local_rows // 2
    positions = keys.shape[1]
    last = len(phases) - 1
    starts = [sum(phases[:i]) * HEAD_SIZE for i in range(len(phases))]
    widths = [heads * HEAD_SIZE for heads in phases]
    nc = len(chunks)
    q_starts = [sum(chunks[:i]) * HEAD_SIZE for i in range(nc)]
    q_widths = [heads * HEAD_SIZE for heads in chunks]
    me = lax.axis_index("gx")
    my = lax.axis_index("gy")
    leader = lax.rem(my, 2) == 1
    follower = lax.rem(my, 2) == 0

    small = [
        pltpu.make_async_copy(tok_hbm, tok, small_sem.at[0]),
        pltpu.make_async_copy(gain_hbm, gain, small_sem.at[1]),
        pltpu.make_async_copy(freq_hbm, freq, small_sem.at[2]),
        pltpu.make_async_copy(lens_hbm, lens, small_sem.at[3]),
    ]

    pieces = [(wk_hbm, wk)]
    for c in range(nc):
        for begin, end in splits[c]:
            at = (pl.ds(begin, end - begin), pl.ds(q_starts[c], q_widths[c]))
            pieces.append((wq_hbm.at[at], wq.at[at]))

    for r in range(local_rows):
        at = pl.ds(r * 2 * positions, 2 * positions)
        pieces.append((kv_hbm.at[at], kv.at[at]))

    def stream(i):
        return pltpu.make_async_copy(*pieces[i], stream_sem.at[i % ahead])

    def take(i):
        stream(i).wait()
        if i + ahead < len(pieces):
            stream(i + ahead).start()

    def wo_copy(c):
        at = pl.ds(starts[c], widths[c])
        return pltpu.make_async_copy(wo_hbm.at[at], wo.at[at], small_sem.at[c])

    for copy in small:
        copy.start()
    for i in range(ahead):
        stream(i).start()

    barrier = pltpu.get_barrier_semaphore()

    def each(fn):
        if n <= 8:
            for d in range(1, n):
                fn(d)
        else:
            def body(d, carry):
                fn(d)
                return carry
            lax.fori_loop(1, n, body, 0)

    def greet(d):
        pl.semaphore_signal(
            barrier, inc=1, device_id={"gx": lax.rem(me + d, n)}, device_id_type=MESH
        )

    each(greet)

    for d in range(1, ny):
        pl.semaphore_signal(
            barrier, inc=1, device_id={"gy": lax.rem(my + d, ny)}, device_id_type=MESH
        )

    def to(d):
        return lax.rem(me + d, n)

    def drain(ref, sem):
        pltpu.make_async_copy(ref, ref, sem).wait()

    small[0].wait()
    small[1].wait()
    x = tok[...].astype(jnp.float32).reshape(total_rows, depth)
    for k in range(depth // HEAD_SIZE):
        cols = slice(k * HEAD_SIZE, (k + 1) * HEAD_SIZE)
        normed[:, cols] = (x[:, cols] * gain[k:k + 1, :].astype(jnp.float32)).astype(jnp.bfloat16)
    squares = jnp.broadcast_to(jnp.sum(x * x, axis=1, keepdims=True), (total_rows, HEAD_SIZE))

    def put(part, start):
        width = part.shape[1]
        for j in range(n):
            for b in range(batches):
                send[j, b * here:(b + 1) * here, start:start + width] = part[
                    b * rows + j * here:b * rows + (j + 1) * here, :
                ]

    def put_halves(start, width):
        for j in range(n):
            for b in range(batches):
                at = slice(b * rows + j * here, b * rows + (j + 1) * here)
                send[j, b * here:(b + 1) * here, start:start + width] = (
                    acc[at, :width] + acc[at, width:2 * width]
                )

    def stage(start):
        return sum(start >= begin for begin in starts[1:] + [q_width])

    def shift(start, width):
        cols = pl.ds(start, width)
        def one(d):
            pltpu.make_async_remote_copy(
                src_ref=send.at[to(d), :, cols], dst_ref=recv.at[me, :, cols],
                send_sem=qs_sem, recv_sem=qr_sem.at[stage(start)],
                device_id={"gx": to(d)}, device_id_type=MESH,
            ).start()
        each(one)

    def arrived(c, start, width):
        drain(recv.at[pl.ds(0, n - 1), :, pl.ds(start, width)], qr_sem.at[c])

    def summed(start, width):
        cols = pl.ds(start, width)
        def add(d, acc):
            return acc + recv[to(d), :, cols]
        return lax.fori_loop(1, n, add, send[me, :, cols], unroll=n <= 8)

    side = kv_width + HEAD_SIZE
    take(0)
    middle = depth // 2
    for k in range(2):
        ks = slice(k * middle, (k + 1) * middle)
        acc[:, k * kv_width:(k + 1) * kv_width] = jnp.dot(
            normed[:, ks], wk[ks], preferred_element_type=jnp.float32
        )
    put_halves(q_width, kv_width)
    put(squares, q_width + kv_width)
    i = 1
    for c in range(nc):
        for k, (begin, end) in enumerate(splits[c]):
            take(i)
            i += 1
            narrow = q_widths[c] == 2 * HEAD_SIZE
            half = q_widths[c] if narrow else q_widths[c] // 2
            size = (end - begin) // 2 if narrow else end - begin
            for m in range(2):
                at = 0 if narrow else m * half
                ks = slice(begin + m * size, begin + (m + 1) * size) if narrow else slice(begin, end)
                piece = jnp.dot(
                    normed[:, ks], wq[ks, q_starts[c] + at:q_starts[c] + at + half],
                    preferred_element_type=jnp.float32,
                )
                into = slice(m * half, (m + 1) * half)
                if k > 0:
                    piece = piece + acc[:, into]
                if narrow or k < len(splits[c]) - 1:
                    acc[:, into] = piece
                else:
                    put(piece, q_starts[c] + at)
        if narrow:
            put_halves(q_starts[c], half)
        if c == 0:
            pl.semaphore_wait(barrier, n - 1 + ny - 1)
            shift(q_width, side)
        shift(q_starts[c], q_widths[c])

    small[2].wait()
    small[3].wait()
    lane = lax.broadcasted_iota(jnp.int32, (local_rows, HEAD_SIZE), 1)
    row = lax.broadcasted_iota(jnp.int32, (local_rows, HEAD_SIZE), 0)
    place = jnp.zeros((local_rows, HEAD_SIZE), jnp.float32)
    for r in range(local_rows):
        place = jnp.where(row == r, lens[r // here, r % here].astype(jnp.float32), place)
    angle = place * freq[...]
    cosine = jnp.cos(angle)
    sine = jnp.sin(angle)
    sine = jnp.where(lane < HEAD_SIZE // 2, -sine, sine)

    def rotate(v):
        return v * cosine + pltpu.roll(v, HEAD_SIZE // 2, 1) * sine

    block_rows = wide_s.shape[1]
    blocks = 2 * positions // block_rows
    half_rows = block_rows // 2

    def divide(r):
        lanes = slice((r % 2) * HEAD_SIZE, (r % 2 + 1) * HEAD_SIZE)
        for t in range(blocks):
            start = (r * blocks + t) * block_rows
            wide = wide_s.at[t % 2]
            wide[...] = kv[start:start + block_rows, :].astype(jnp.float32)
            at = slice(t * half_rows, (t + 1) * half_rows)
            keys[r // 2, at, lanes] = wide[pl.ds(0, half_rows, stride=2), :].astype(jnp.bfloat16)
            values[r // 2, at, lanes] = wide[pl.ds(1, half_rows, stride=2), :].astype(jnp.bfloat16)

    def prepare(c):
        hc = phases[c]
        arrived(c, starts[c], widths[c])
        block = summed(starts[c], widths[c])
        for h in range(hc):
            q_s[pl.ds(h, local_rows, stride=hc), :] = rotate(
                block[:, h * HEAD_SIZE:(h + 1) * HEAD_SIZE] * scale
            )

    for r in range(local_rows // 2):
        take(i)
        i += 1
        divide(r)
    wo_copy(0).start()
    arrived(last + 1, q_width, side)
    tail = summed(q_width, side)
    scale = lax.rsqrt(tail[:, kv_width:] / MODEL_WIDTH + 1e-05)
    rkey = rotate(tail[:, :HEAD_SIZE] * scale)
    value_new = tail[:, HEAD_SIZE:2 * HEAD_SIZE] * scale
    prepare(0)
    for r in range(local_rows // 2, local_rows):
        take(i)
        i += 1
        if r == local_rows - 1:
            for c in range(1, last + 1):
                wo_copy(c).start()
        divide(r)
    inv_root = np.float32(1.0 / np.sqrt(np.float32(HEAD_SIZE)))

    def spread(c):
        cols = pl.ds(starts[c], widths[c])
        def one(d):
            pltpu.make_async_remote_copy(
                src_ref=att_send.at[:, cols], dst_ref=att_recv.at[me, :, cols],
                send_sem=as_sem, recv_sem=ar_sem.at[c],
                device_id={"gx": to(d)}, device_id_type=MESH,
            ).start()
        each(one)

    for c in range(last + 1):
        hc = phases[c]
        if c > 0:
            prepare(c)
        column = lax.broadcasted_iota(jnp.int32, (2 * hc, positions), 1)
        first = lax.broadcasted_iota(jnp.int32, (2 * hc, HEAD_SIZE), 0) < hc
        first_wide = lax.broadcasted_iota(jnp.int32, (2 * hc, positions), 0) < hc

        def pair_rows(v, p):
            shape = (2 * hc, v.shape[1])
            return jnp.where(
                first,
                jnp.broadcast_to(v[2 * p:2 * p + 1], shape),
                jnp.broadcast_to(v[2 * p + 1:2 * p + 2], shape),
            )

        weighed = []
        for p in range(pairs):
            query = q_s[p * 2 * hc:(p + 1) * 2 * hc, :].astype(jnp.bfloat16).astype(jnp.float32)
            both = jnp.concatenate(
                [jnp.where(first, query, 0.0), jnp.where(first, 0.0, query)], axis=1
            ).astype(jnp.bfloat16)
            scores = jnp.concatenate(
                [
                    lax.dot_general(
                        both, keys[p, at:at + positions // 2], (((1,), (1,)), ((), ())),
                        preferred_element_type=jnp.float32,
                    )
                    for at in (0, positions // 2)
                ],
                axis=1,
            ) * inv_root
            r = 2 * p
            limit = jnp.where(
                first_wide, lens[r // here, r % here], lens[(r + 1) // here, (r + 1) % here]
            )
            scores = jnp.where(column < limit, scores, -1e30)
            new_score = jnp.sum(query * pair_rows(rkey, p), axis=1, keepdims=True) * inv_root
            top = jnp.maximum(jnp.max(scores, axis=1, keepdims=True), new_score)
            weights = jnp.exp(scores - top)
            new_weight = jnp.exp(new_score - top)
            total = jnp.sum(weights, axis=1, keepdims=True) + new_weight
            weighed.append((weights.astype(jnp.bfloat16), new_weight, total))
        for p in range(pairs):
            weights, new_weight, total = weighed[p]
            mixed = sum(
                jnp.dot(
                    weights[:, at:at + positions // 2], values[p, at:at + positions // 2],
                    preferred_element_type=jnp.float32,
                )
                for at in (0, positions // 2)
            )
            mixed = jnp.where(first, mixed[:, :HEAD_SIZE], mixed[:, HEAD_SIZE:])
            o_s[p * 2 * hc:(p + 1) * 2 * hc, :] = (
                mixed + new_weight * pair_rows(value_new, p)
            ) / total
        for h in range(hc):
            cols = slice(starts[c] + h * HEAD_SIZE, starts[c] + (h + 1) * HEAD_SIZE)
            att_send[:, cols] = o_s[pl.ds(h, local_rows, stride=hc), :].astype(jnp.bfloat16)
        spread(c)

    partner = my + 1 - 2 * lax.rem(my, 2)
    far = lax.rem(my + 2, 4)
    far_leader = far + 1 - lax.rem(far, 2)
    far_other = far + 1 - 2 * lax.rem(far, 2)
    final = len(outs) - 1
    final_cols = pl.ds(*outs[final])
    early_cols = pl.ds(0, outs[final][0])

    def hand(o, slot, target):
        cols = pl.ds(*outs[o])
        return pltpu.make_async_remote_copy(
            src_ref=y_send.at[:, cols], dst_ref=y_recv.at[slot, :, cols],
            send_sem=ys_sem.at[o // final if final else 1], recv_sem=yr_sem.at[o],
            device_id={"gy": target}, device_id_type=MESH,
        )

    def give(o):
        cols = pl.ds(*outs[o])
        return pltpu.make_async_remote_copy(
            src_ref=out.at[:, :, cols], dst_ref=out.at[:, :, cols],
            send_sem=out_sem, recv_sem=out_sem,
            device_id={"gy": partner}, device_id_type=MESH,
        )

    def product(o, fs, xc):
        start, width = outs[o]
        for at in (start, start + width // 2):
            part = slice(at, at + width // 2)
            yield part, jnp.dot(xc, wo[fs, part], preferred_element_type=jnp.float32)

    for c in range(last + 1):
        fs = slice(starts[c], starts[c] + widths[c])
        drain(att_recv.at[pl.ds(0, n - 1), :, pl.ds(starts[c], widths[c])], ar_sem.at[c])
        att_recv[me, :, fs] = att_send[:, fs]
        for j in range(n):
            block = att_recv[j, :, fs].astype(jnp.float32)
            for b in range(batches):
                x_s[b * rows + j * here:b * rows + (j + 1) * here, :widths[c]] = block[
                    b * here:(b + 1) * here, :
                ]
        xc = x_s[:, :widths[c]].astype(jnp.bfloat16)
        wo_copy(c).wait()
        if c < last:
            for o in range(len(outs)):
                for part, y in product(o, fs, xc):
                    ybuf[:, part] = y + ybuf[:, part] if c > 0 else y

    for o in range(len(outs)):
        for part, y in product(o, fs, xc):
            y_send[:, part] = (y + ybuf[:, part]).astype(jnp.bfloat16)
        if o < final:
            hand(o, 1 - lax.rem(my, 2), far_leader).start()
        else:
            hand(o, 0, far).start()
            hand(o, 1, far_other).start()
            hand(o, 2, partner).start()

    def total(o):
        cols = slice(outs[o][0], outs[o][0] + outs[o][1])
        drain(y_recv.at[:, :, cols], yr_sem.at[o])
        parts = [y_recv[slot, :, cols].astype(jnp.float32) for slot in range(3)]
        y = (y_send[:, cols].astype(jnp.float32) + parts[0]) + (parts[1] + parts[2])
        y = y.reshape(batches, rows, outs[o][1])
        out[:, :, cols] = (tok[:, :, cols].astype(jnp.float32) + y).astype(jnp.bfloat16)

    if final:
        @pl.when(leader)
        def _():
            for o in range(final):
                total(o)
                give(o).start()

        @pl.when(follower)
        def _():
            for o in range(final):
                hand(o, 2, partner).start()

    total(final)
    if final:
        @pl.when(leader)
        def _():
            drain(y_send.at[:, early_cols], ys_sem.at[0])

        @pl.when(follower)
        def _():
            drain(y_recv.at[0:2, :, early_cols], ys_sem.at[0])

        drain(out.at[:, :, early_cols], out_sem)
    drain(y_recv.at[:, :, final_cols], ys_sem.at[1])
    drain(send.at[pl.ds(0, n - 1)], qs_sem)
    drain(att_recv.at[pl.ds(0, n - 1)], as_sem)


def local(n, ny, tokens, lengths, norm_gain, w_query, key_value_weight, w_out, cache):
    batches, rows, depth = tokens.shape
    here = rows // n
    local_rows = batches * here
    q_width = w_query.shape[1]
    kv_heads = key_value_weight.shape[1]
    kv_width = kv_heads * key_value_weight.shape[2]
    assert kv_heads == 1 and ny == 4 and local_rows % 2 == 0
    heads = q_width // HEAD_SIZE
    out_width = w_out.shape[1]
    quarter = heads // 4
    chunks = (quarter,) * 3 + (quarter // 2,) * 2
    phases = (2 * quarter, 2 * quarter)
    cuts = []
    for c, width in enumerate(chunks):
        parts = max(1, depth * width * HEAD_SIZE >> 20)
        size = depth // parts
        cut = [(k * size, (k + 1) * size) for k in range(parts)]
        if c == len(chunks) - 1 and size % 512 == 0:
            begin, end = cut.pop()
            middle = begin + (end - begin) * 3 // 4
            cut += [(begin, middle), (middle, end)]
        cuts.append(cut)
    ahead = 5
    step = min(1024, out_width)
    outs = [(start, step) for start in range(0, out_width, step)]
    freq = np.float32(ROPE_BASE) ** (
        -2.0 * np.arange(HEAD_SIZE // 2, dtype=np.float32) / HEAD_SIZE
    )
    freq = np.concatenate([freq, freq]).astype(np.float32)[None, :]
    positions = cache.shape[2]
    interleaved = cache.reshape(local_rows * positions * 2, HEAD_SIZE)
    hbm = pl.BlockSpec(memory_space=pltpu.HBM)
    f32, bf16 = jnp.float32, jnp.bfloat16
    dma = pltpu.SemaphoreType.DMA
    total_rows = batches * rows
    wide = q_width + kv_width + HEAD_SIZE
    most = max(phases)
    return pl.pallas_call(
        functools.partial(kernel, n, ny, chunks, cuts, phases, ahead, outs),
        out_shape=pltpu.VMEM(tokens.shape, bf16),
        in_specs=[hbm] * 8,
        out_specs=pl.BlockSpec(memory_space=pltpu.VMEM),
        scratch_shapes=[
            pltpu.SMEM(lengths.shape, jnp.int32),
            pltpu.VMEM(tokens.shape, bf16),
            pltpu.VMEM((depth // HEAD_SIZE, HEAD_SIZE), bf16),
            pltpu.VMEM((1, HEAD_SIZE), f32),
            pltpu.VMEM(w_query.shape, bf16),
            pltpu.VMEM((depth, kv_width), bf16),
            pltpu.VMEM(w_out.shape, bf16),
            pltpu.VMEM(interleaved.shape, bf16),
            pltpu.VMEM((total_rows, depth), bf16),
            pltpu.VMEM((total_rows, most * HEAD_SIZE), f32),
            pltpu.VMEM((2, positions, HEAD_SIZE), f32),
            pltpu.VMEM((local_rows // 2, positions, 2 * HEAD_SIZE), bf16),
            pltpu.VMEM((local_rows // 2, positions, 2 * HEAD_SIZE), bf16),
            pltpu.VMEM((n, local_rows, wide), f32),
            pltpu.VMEM((n, local_rows, wide), f32),
            pltpu.VMEM((local_rows * most, HEAD_SIZE), f32),
            pltpu.VMEM((local_rows * most, HEAD_SIZE), f32),
            pltpu.VMEM((local_rows, q_width), bf16),
            pltpu.VMEM((n, local_rows, q_width), bf16),
            pltpu.VMEM((total_rows, most * HEAD_SIZE), f32),
            pltpu.VMEM((total_rows, out_width), f32),
            pltpu.VMEM((total_rows, out_width), bf16),
            pltpu.VMEM((3, total_rows, out_width), bf16),
            dma((4,)), dma((ahead,)), dma, dma((len(phases) + 1,)),
            dma, dma((len(phases),)), dma((2,)), dma((len(outs),)), dma,
        ],
        compiler_params=pltpu.CompilerParams(
            collective_id=0, has_side_effects=True, vmem_limit_bytes=67043328 - 2 * tokens.size
        ),
    )(
        lengths, tokens, norm_gain.reshape(depth // HEAD_SIZE, HEAD_SIZE), jnp.asarray(freq),
        w_query, key_value_weight.reshape(depth, kv_width), w_out, interleaved,
    )


def solution(mesh):
    placed = (
        P(None, "groups", "gx"),
        P(None, ("groups", "gx")),
        P("gx"),
        P("gx", "gy"),
        P("gx", "gy", None),
        P("gy", "gx"),
        P(None, ("groups", "gx"), None, "gy", None, None),
    )
    return jax.shard_map(
        functools.partial(local, mesh.shape["gx"], mesh.shape["gy"]),
        mesh=mesh, in_specs=placed, out_specs=P(None, "groups", "gx"), check_vma=False,
    )
```

```python
import functools

import jax
import jax.numpy as jnp
import numpy as np
from jax import lax
from jax.experimental import pallas as pl
from jax.experimental.pallas import tpu as pltpu
from jax.sharding import PartitionSpec as P

MODEL_WIDTH = 16384
HEAD_SIZE = 128
ROPE_BASE = 500000.0
MESH = pl.DeviceIdType.MESH


def kernel(
    n, ny, chunks, splits, phases, ahead, outs,
    lens_hbm, tok_hbm, gain_hbm, freq_hbm, wq_hbm, wk_hbm, wo_hbm, kv_hbm,
    out,
    lens, tok, gain, freq, wq, wk, wo, kv, normed,
    acc, wide_s, keys, values, send, recv, q_s, o_s, att_send, att_recv, x_s,
    ybuf, y_send, y_recv,
    small_sem, stream_sem, qs_sem, qr_sem, as_sem, ar_sem, ys_sem, yr_sem, out_sem,
):
    batches, rows, depth = tok.shape
    here = rows // n
    total_rows = batches * rows
    q_width = wq.shape[1]
    kv_width = wk.shape[1]
    out_width = wo.shape[1]
    local_rows = batches * here
    pairs = local_rows // 2
    positions = keys.shape[1]
    last = len(phases) - 1
    starts = [sum(phases[:i]) * HEAD_SIZE for i in range(len(phases))]
    widths = [heads * HEAD_SIZE for heads in phases]
    nc = len(chunks)
    q_starts = [sum(chunks[:i]) * HEAD_SIZE for i in range(nc)]
    q_widths = [heads * HEAD_SIZE for heads in chunks]
    me = lax.axis_index("gx")
    my = lax.axis_index("gy")
    leader = lax.rem(my, 2) == 1
    follower = lax.rem(my, 2) == 0

    small = [
        pltpu.make_async_copy(tok_hbm, tok, small_sem.at[0]),
        pltpu.make_async_copy(gain_hbm, gain, small_sem.at[1]),
        pltpu.make_async_copy(freq_hbm, freq, small_sem.at[2]),
        pltpu.make_async_copy(lens_hbm, lens, small_sem.at[3]),
    ]

    pieces = [(wk_hbm, wk)]
    for c in range(nc):
        for begin, end in splits[c]:
            at = (pl.ds(begin, end - begin), pl.ds(q_starts[c], q_widths[c]))
            pieces.append((wq_hbm.at[at], wq.at[at]))

    for r in range(local_rows):
        at = pl.ds(r * 2 * positions, 2 * positions)
        pieces.append((kv_hbm.at[at], kv.at[at]))

    def stream(i):
        return pltpu.make_async_copy(*pieces[i], stream_sem.at[i % ahead])

    def take(i):
        stream(i).wait()
        if i + ahead < len(pieces):
            stream(i + ahead).start()

    def wo_copy(c):
        at = pl.ds(starts[c], widths[c])
        return pltpu.make_async_copy(wo_hbm.at[at], wo.at[at], small_sem.at[c])

    for copy in small:
        copy.start()
    for i in range(ahead):
        stream(i).start()

    barrier = pltpu.get_barrier_semaphore()

    def each(fn):
        if n <= 8:
            for d in range(1, n):
                fn(d)
        else:
            def body(d, carry):
                fn(d)
                return carry
            lax.fori_loop(1, n, body, 0)

    def greet(d):
        pl.semaphore_signal(
            barrier, inc=1, device_id={"gx": lax.rem(me + d, n)}, device_id_type=MESH
        )

    each(greet)

    for d in range(1, ny):
        pl.semaphore_signal(
            barrier, inc=1, device_id={"gy": lax.rem(my + d, ny)}, device_id_type=MESH
        )

    def to(d):
        return lax.rem(me + d, n)

    def drain(ref, sem):
        pltpu.make_async_copy(ref, ref, sem).wait()

    small[0].wait()
    small[1].wait()
    x = tok[...].astype(jnp.float32).reshape(total_rows, depth)
    for k in range(depth // HEAD_SIZE):
        cols = slice(k * HEAD_SIZE, (k + 1) * HEAD_SIZE)
        normed[:, cols] = (x[:, cols] * gain[k:k + 1, :].astype(jnp.float32)).astype(jnp.bfloat16)
    squares = jnp.broadcast_to(jnp.sum(x * x, axis=1, keepdims=True), (total_rows, HEAD_SIZE))

    def put(part, start):
        width = part.shape[1]
        for j in range(n):
            for b in range(batches):
                send[j, b * here:(b + 1) * here, start:start + width] = part[
                    b * rows + j * here:b * rows + (j + 1) * here, :
                ]

    def put_halves(start, width):
        for j in range(n):
            for b in range(batches):
                at = slice(b * rows + j * here, b * rows + (j + 1) * here)
                send[j, b * here:(b + 1) * here, start:start + width] = (
                    acc[at, :width] + acc[at, width:2 * width]
                )

    def stage(start):
        return sum(start >= begin for begin in starts[1:] + [q_width])

    def shift(start, width):
        cols = pl.ds(start, width)
        def one(d):
            pltpu.make_async_remote_copy(
                src_ref=send.at[to(d), :, cols], dst_ref=recv.at[me, :, cols],
                send_sem=qs_sem, recv_sem=qr_sem.at[stage(start)],
                device_id={"gx": to(d)}, device_id_type=MESH,
            ).start()
        each(one)

    def arrived(c, start, width):
        drain(recv.at[pl.ds(0, n - 1), :, pl.ds(start, width)], qr_sem.at[c])

    def summed(start, width):
        cols = pl.ds(start, width)
        def add(d, acc):
            return acc + recv[to(d), :, cols]
        return lax.fori_loop(1, n, add, send[me, :, cols], unroll=n <= 8)

    side = kv_width + HEAD_SIZE
    take(0)
    middle = depth // 2
    for k in range(2):
        ks = slice(k * middle, (k + 1) * middle)
        acc[:, k * kv_width:(k + 1) * kv_width] = jnp.dot(
            normed[:, ks], wk[ks], preferred_element_type=jnp.float32
        )
    put_halves(q_width, kv_width)
    put(squares, q_width + kv_width)
    i = 1
    for c in range(nc):
        for k, (begin, end) in enumerate(splits[c]):
            take(i)
            i += 1
            narrow = q_widths[c] == 2 * HEAD_SIZE
            half = q_widths[c] if narrow else q_widths[c] // 2
            size = (end - begin) // 2 if narrow else end - begin
            for m in range(2):
                at = 0 if narrow else m * half
                ks = slice(begin + m * size, begin + (m + 1) * size) if narrow else slice(begin, end)
                piece = jnp.dot(
                    normed[:, ks], wq[ks, q_starts[c] + at:q_starts[c] + at + half],
                    preferred_element_type=jnp.float32,
                )
                into = slice(m * half, (m + 1) * half)
                if k > 0:
                    piece = piece + acc[:, into]
                if narrow or k < len(splits[c]) - 1:
                    acc[:, into] = piece
                else:
                    put(piece, q_starts[c] + at)
        if narrow:
            put_halves(q_starts[c], half)
        if c == 0:
            pl.semaphore_wait(barrier, n - 1 + ny - 1)
            shift(q_width, side)
        shift(q_starts[c], q_widths[c])

    small[2].wait()
    small[3].wait()
    lane = lax.broadcasted_iota(jnp.int32, (local_rows, HEAD_SIZE), 1)
    row = lax.broadcasted_iota(jnp.int32, (local_rows, HEAD_SIZE), 0)
    place = jnp.zeros((local_rows, HEAD_SIZE), jnp.float32)
    for r in range(local_rows):
        place = jnp.where(row == r, lens[r // here, r % here].astype(jnp.float32), place)
    angle = place * freq[...]
    cosine = jnp.cos(angle)
    sine = jnp.sin(angle)
    sine = jnp.where(lane < HEAD_SIZE // 2, -sine, sine)

    def rotate(v):
        return v * cosine + pltpu.roll(v, HEAD_SIZE // 2, 1) * sine

    block_rows = wide_s.shape[1]
    blocks = 2 * positions // block_rows
    half_rows = block_rows // 2

    def divide(r):
        lanes = slice((r % 2) * HEAD_SIZE, (r % 2 + 1) * HEAD_SIZE)
        for t in range(blocks):
            start = (r * blocks + t) * block_rows
            wide = wide_s.at[t % 2]
            wide[...] = kv[start:start + block_rows, :].astype(jnp.float32)
            at = slice(t * half_rows, (t + 1) * half_rows)
            keys[r // 2, at, lanes] = wide[pl.ds(0, half_rows, stride=2), :].astype(jnp.bfloat16)
            values[r // 2, at, lanes] = wide[pl.ds(1, half_rows, stride=2), :].astype(jnp.bfloat16)

    def prepare(c):
        hc = phases[c]
        arrived(c, starts[c], widths[c])
        block = summed(starts[c], widths[c])
        for h in range(hc):
            q_s[pl.ds(h, local_rows, stride=hc), :] = rotate(
                block[:, h * HEAD_SIZE:(h + 1) * HEAD_SIZE] * scale
            )

    for r in range(local_rows // 2):
        take(i)
        i += 1
        divide(r)
    wo_copy(0).start()
    arrived(last + 1, q_width, side)
    tail = summed(q_width, side)
    scale = lax.rsqrt(tail[:, kv_width:] / MODEL_WIDTH + 1e-05)
    rkey = rotate(tail[:, :HEAD_SIZE] * scale)
    value_new = tail[:, HEAD_SIZE:2 * HEAD_SIZE] * scale
    prepare(0)
    for r in range(local_rows // 2, local_rows):
        take(i)
        i += 1
        if r == local_rows - 1:
            for c in range(1, last + 1):
                wo_copy(c).start()
        divide(r)
    inv_root = np.float32(1.0 / np.sqrt(np.float32(HEAD_SIZE)))

    def spread(c):
        cols = pl.ds(starts[c], widths[c])
        def one(d):
            pltpu.make_async_remote_copy(
                src_ref=att_send.at[:, cols], dst_ref=att_recv.at[me, :, cols],
                send_sem=as_sem, recv_sem=ar_sem.at[c],
                device_id={"gx": to(d)}, device_id_type=MESH,
            ).start()
        each(one)

    for c in range(last + 1):
        hc = phases[c]
        if c > 0:
            prepare(c)
        column = lax.broadcasted_iota(jnp.int32, (2 * hc, positions), 1)
        first = lax.broadcasted_iota(jnp.int32, (2 * hc, HEAD_SIZE), 0) < hc
        first_wide = lax.broadcasted_iota(jnp.int32, (2 * hc, positions), 0) < hc

        def pair_rows(v, p):
            shape = (2 * hc, v.shape[1])
            return jnp.where(
                first,
                jnp.broadcast_to(v[2 * p:2 * p + 1], shape),
                jnp.broadcast_to(v[2 * p + 1:2 * p + 2], shape),
            )

        weighed = []
        for p in range(pairs):
            query = q_s[p * 2 * hc:(p + 1) * 2 * hc, :].astype(jnp.bfloat16).astype(jnp.float32)
            both = jnp.concatenate(
                [jnp.where(first, query, 0.0), jnp.where(first, 0.0, query)], axis=1
            ).astype(jnp.bfloat16)
            scores = jnp.concatenate(
                [
                    lax.dot_general(
                        both, keys[p, at:at + positions // 2], (((1,), (1,)), ((), ())),
                        preferred_element_type=jnp.float32,
                    )
                    for at in (0, positions // 2)
                ],
                axis=1,
            ) * inv_root
            r = 2 * p
            limit = jnp.where(
                first_wide, lens[r // here, r % here], lens[(r + 1) // here, (r + 1) % here]
            )
            scores = jnp.where(column < limit, scores, -1e30)
            new_score = jnp.sum(query * pair_rows(rkey, p), axis=1, keepdims=True) * inv_root
            top = jnp.maximum(jnp.max(scores, axis=1, keepdims=True), new_score)
            weights = jnp.exp(scores - top)
            new_weight = jnp.exp(new_score - top)
            total = jnp.sum(weights, axis=1, keepdims=True) + new_weight
            weighed.append((weights.astype(jnp.bfloat16), new_weight, total))
        for p in range(pairs):
            weights, new_weight, total = weighed[p]
            mixed = sum(
                jnp.dot(
                    weights[:, at:at + positions // 2], values[p, at:at + positions // 2],
                    preferred_element_type=jnp.float32,
                )
                for at in (0, positions // 2)
            )
            mixed = jnp.where(first, mixed[:, :HEAD_SIZE], mixed[:, HEAD_SIZE:])
            o_s[p * 2 * hc:(p + 1) * 2 * hc, :] = (
                mixed + new_weight * pair_rows(value_new, p)
            ) / total
        for h in range(hc):
            cols = slice(starts[c] + h * HEAD_SIZE, starts[c] + (h + 1) * HEAD_SIZE)
            att_send[:, cols] = o_s[pl.ds(h, local_rows, stride=hc), :].astype(jnp.bfloat16)
        spread(c)

    partner = my + 1 - 2 * lax.rem(my, 2)
    far = lax.rem(my + 2, 4)
    far_leader = far + 1 - lax.rem(far, 2)
    far_other = far + 1 - 2 * lax.rem(far, 2)
    final = len(outs) - 1
    final_cols = pl.ds(*outs[final])
    early_cols = pl.ds(0, outs[final][0])

    def hand(o, slot, target):
        cols = pl.ds(*outs[o])
        return pltpu.make_async_remote_copy(
            src_ref=y_send.at[:, cols], dst_ref=y_recv.at[slot, :, cols],
            send_sem=ys_sem.at[o // final if final else 1], recv_sem=yr_sem.at[o],
            device_id={"gy": target}, device_id_type=MESH,
        )

    def give(o):
        cols = pl.ds(*outs[o])
        return pltpu.make_async_remote_copy(
            src_ref=out.at[:, :, cols], dst_ref=out.at[:, :, cols],
            send_sem=out_sem, recv_sem=out_sem,
            device_id={"gy": partner}, device_id_type=MESH,
        )

    def product(o, fs, xc):
        start, width = outs[o]
        for at in (start, start + width // 2):
            part = slice(at, at + width // 2)
            yield part, jnp.dot(xc, wo[fs, part], preferred_element_type=jnp.float32)

    for c in range(last + 1):
        fs = slice(starts[c], starts[c] + widths[c])
        drain(att_recv.at[pl.ds(0, n - 1), :, pl.ds(starts[c], widths[c])], ar_sem.at[c])
        att_recv[me, :, fs] = att_send[:, fs]
        for j in range(n):
            block = att_recv[j, :, fs].astype(jnp.float32)
            for b in range(batches):
                x_s[b * rows + j * here:b * rows + (j + 1) * here, :widths[c]] = block[
                    b * here:(b + 1) * here, :
                ]
        xc = x_s[:, :widths[c]].astype(jnp.bfloat16)
        wo_copy(c).wait()
        if c < last:
            for o in range(len(outs)):
                for part, y in product(o, fs, xc):
                    ybuf[:, part] = y + ybuf[:, part] if c > 0 else y

    for o in range(len(outs)):
        for part, y in product(o, fs, xc):
            y_send[:, part] = (y + ybuf[:, part]).astype(jnp.bfloat16)
        if o < final:
            hand(o, 1 - lax.rem(my, 2), far_leader).start()
        else:
            hand(o, 0, far).start()
            hand(o, 1, far_other).start()
            hand(o, 2, partner).start()

    def total(o):
        cols = slice(outs[o][0], outs[o][0] + outs[o][1])
        drain(y_recv.at[:, :, cols], yr_sem.at[o])
        parts = [y_recv[slot, :, cols].astype(jnp.float32) for slot in range(3)]
        y = (y_send[:, cols].astype(jnp.float32) + parts[0]) + (parts[1] + parts[2])
        y = y.reshape(batches, rows, outs[o][1])
        out[:, :, cols] = (tok[:, :, cols].astype(jnp.float32) + y).astype(jnp.bfloat16)

    if final:
        @pl.when(leader)
        def _():
            for o in range(final):
                total(o)
                give(o).start()

        @pl.when(follower)
        def _():
            for o in range(final):
                hand(o, 2, partner).start()

    total(final)
    if final:
        @pl.when(leader)
        def _():
            drain(y_send.at[:, early_cols], ys_sem.at[0])

        @pl.when(follower)
        def _():
            drain(y_recv.at[0:2, :, early_cols], ys_sem.at[0])

        drain(out.at[:, :, early_cols], out_sem)
    drain(y_recv.at[:, :, final_cols], ys_sem.at[1])
    drain(send.at[pl.ds(0, n - 1)], qs_sem)
    drain(att_recv.at[pl.ds(0, n - 1)], as_sem)


def local(n, ny, tokens, lengths, norm_gain, w_query, key_value_weight, w_out, cache):
    batches, rows, depth = tokens.shape
    here = rows // n
    local_rows = batches * here
    q_width = w_query.shape[1]
    kv_heads = key_value_weight.shape[1]
    kv_width = kv_heads * key_value_weight.shape[2]
    assert kv_heads == 1 and ny == 4 and local_rows % 2 == 0
    heads = q_width // HEAD_SIZE
    out_width = w_out.shape[1]
    quarter = heads // 4
    chunks = (quarter,) * 3 + (quarter // 2,) * 2
    phases = (2 * quarter, 2 * quarter)
    cuts = []
    for c, width in enumerate(chunks):
        parts = max(1, depth * width * HEAD_SIZE >> 20)
        size = depth // parts
        cut = [(k * size, (k + 1) * size) for k in range(parts)]
        if c == len(chunks) - 1 and size % 512 == 0:
            begin, end = cut.pop()
            middle = begin + (end - begin) * 3 // 4
            cut += [(begin, middle), (middle, end)]
        cuts.append(cut)
    ahead = 5
    blocks = (2, 3, 3)
    eighth = out_width // 8
    outs = [(0, out_width)]
    if eighth % (2 * HEAD_SIZE) == 0:
        outs = [(sum(blocks[:o]) * eighth, blocks[o] * eighth) for o in range(len(blocks))]
    freq = np.float32(ROPE_BASE) ** (
        -2.0 * np.arange(HEAD_SIZE // 2, dtype=np.float32) / HEAD_SIZE
    )
    freq = np.concatenate([freq, freq]).astype(np.float32)[None, :]
    positions = cache.shape[2]
    interleaved = cache.reshape(local_rows * positions * 2, HEAD_SIZE)
    hbm = pl.BlockSpec(memory_space=pltpu.HBM)
    f32, bf16 = jnp.float32, jnp.bfloat16
    dma = pltpu.SemaphoreType.DMA
    total_rows = batches * rows
    wide = q_width + kv_width + HEAD_SIZE
    most = max(phases)
    return pl.pallas_call(
        functools.partial(kernel, n, ny, chunks, cuts, phases, ahead, outs),
        out_shape=pltpu.VMEM(tokens.shape, bf16),
        in_specs=[hbm] * 8,
        out_specs=pl.BlockSpec(memory_space=pltpu.VMEM),
        scratch_shapes=[
            pltpu.SMEM(lengths.shape, jnp.int32),
            pltpu.VMEM(tokens.shape, bf16),
            pltpu.VMEM((depth // HEAD_SIZE, HEAD_SIZE), bf16),
            pltpu.VMEM((1, HEAD_SIZE), f32),
            pltpu.VMEM(w_query.shape, bf16),
            pltpu.VMEM((depth, kv_width), bf16),
            pltpu.VMEM(w_out.shape, bf16),
            pltpu.VMEM(interleaved.shape, bf16),
            pltpu.VMEM((total_rows, depth), bf16),
            pltpu.VMEM((total_rows, most * HEAD_SIZE), f32),
            pltpu.VMEM((2, positions, HEAD_SIZE), f32),
            pltpu.VMEM((local_rows // 2, positions, 2 * HEAD_SIZE), bf16),
            pltpu.VMEM((local_rows // 2, positions, 2 * HEAD_SIZE), bf16),
            pltpu.VMEM((n, local_rows, wide), f32),
            pltpu.VMEM((n, local_rows, wide), f32),
            pltpu.VMEM((local_rows * most, HEAD_SIZE), f32),
            pltpu.VMEM((local_rows * most, HEAD_SIZE), f32),
            pltpu.VMEM((local_rows, q_width), bf16),
            pltpu.VMEM((n, local_rows, q_width), bf16),
            pltpu.VMEM((total_rows, most * HEAD_SIZE), f32),
            pltpu.VMEM((total_rows, out_width), f32),
            pltpu.VMEM((total_rows, out_width), bf16),
            pltpu.VMEM((3, total_rows, out_width), bf16),
            dma((4,)), dma((ahead,)), dma, dma((len(phases) + 1,)),
            dma, dma((len(phases),)), dma((2,)), dma((len(outs),)), dma,
        ],
        compiler_params=pltpu.CompilerParams(
            collective_id=0, has_side_effects=True, vmem_limit_bytes=67043328 - 2 * tokens.size
        ),
    )(
        lengths, tokens, norm_gain.reshape(depth // HEAD_SIZE, HEAD_SIZE), jnp.asarray(freq),
        w_query, key_value_weight.reshape(depth, kv_width), w_out, interleaved,
    )


def solution(mesh):
    placed = (
        P(None, "groups", "gx"),
        P(None, ("groups", "gx")),
        P("gx"),
        P("gx", "gy"),
        P("gx", "gy", None),
        P("gy", "gx"),
        P(None, ("groups", "gx"), None, "gy", None, None),
    )
    return jax.shard_map(
        functools.partial(local, mesh.shape["gx"], mesh.shape["gy"]),
        mesh=mesh, in_specs=placed, out_specs=P(None, "groups", "gx"), check_vma=False,
    )
```

```python
import functools

import jax
import jax.numpy as jnp
import numpy as np
from jax import lax
from jax.experimental import pallas as pl
from jax.experimental.pallas import tpu as pltpu
from jax.sharding import PartitionSpec as P

MODEL_WIDTH = 16384
HEAD_SIZE = 128
ROPE_BASE = 500000.0
MESH = pl.DeviceIdType.MESH


def kernel(
    n, ny, chunks, splits, phases, ahead, outs,
    lens_hbm, tok_hbm, gain_hbm, freq_hbm, wq_hbm, wk_hbm, wo_hbm, kv_hbm,
    out,
    lens, tok, gain, freq, wq, wk, wo, kv, normed,
    acc, wide_s, keys, values, send, recv, q_s, o_s, att_send, att_recv, x_s,
    ybuf, y_send, y_recv,
    small_sem, stream_sem, qs_sem, qr_sem, as_sem, ar_sem, ys_sem, yr_sem, out_sem,
):
    batches, rows, depth = tok.shape
    here = rows // n
    total_rows = batches * rows
    q_width = wq.shape[1]
    kv_width = wk.shape[1]
    out_width = wo.shape[1]
    local_rows = batches * here
    pairs = local_rows // 2
    positions = keys.shape[1]
    last = len(phases) - 1
    starts = [sum(phases[:i]) * HEAD_SIZE for i in range(len(phases))]
    widths = [heads * HEAD_SIZE for heads in phases]
    nc = len(chunks)
    q_starts = [sum(chunks[:i]) * HEAD_SIZE for i in range(nc)]
    q_widths = [heads * HEAD_SIZE for heads in chunks]
    me = lax.axis_index("gx")
    my = lax.axis_index("gy")
    leader = lax.rem(my, 2) == 1
    follower = lax.rem(my, 2) == 0

    small = [
        pltpu.make_async_copy(tok_hbm, tok, small_sem.at[0]),
        pltpu.make_async_copy(gain_hbm, gain, small_sem.at[1]),
        pltpu.make_async_copy(freq_hbm, freq, small_sem.at[2]),
        pltpu.make_async_copy(lens_hbm, lens, small_sem.at[3]),
    ]

    pieces = [(wk_hbm, wk)]
    for c in range(nc):
        for begin, end in splits[c]:
            at = (pl.ds(begin, end - begin), pl.ds(q_starts[c], q_widths[c]))
            pieces.append((wq_hbm.at[at], wq.at[at]))

    for r in range(local_rows):
        at = pl.ds(r * 2 * positions, 2 * positions)
        pieces.append((kv_hbm.at[at], kv.at[at]))

    def stream(i):
        return pltpu.make_async_copy(*pieces[i], stream_sem.at[i % ahead])

    def take(i):
        stream(i).wait()
        if i + ahead < len(pieces):
            stream(i + ahead).start()

    def wo_copy(c):
        at = pl.ds(starts[c], widths[c])
        return pltpu.make_async_copy(wo_hbm.at[at], wo.at[at], small_sem.at[c])

    for copy in small:
        copy.start()
    for i in range(ahead):
        stream(i).start()

    barrier = pltpu.get_barrier_semaphore()

    def each(fn):
        if n <= 8:
            for d in range(1, n):
                fn(d)
        else:
            def body(d, carry):
                fn(d)
                return carry
            lax.fori_loop(1, n, body, 0)

    def greet(d):
        pl.semaphore_signal(
            barrier, inc=1, device_id={"gx": lax.rem(me + d, n)}, device_id_type=MESH
        )

    each(greet)

    for d in range(1, ny):
        pl.semaphore_signal(
            barrier, inc=1, device_id={"gy": lax.rem(my + d, ny)}, device_id_type=MESH
        )

    def to(d):
        return lax.rem(me + d, n)

    def drain(ref, sem):
        pltpu.make_async_copy(ref, ref, sem).wait()

    small[0].wait()
    small[1].wait()
    x = tok[...].astype(jnp.float32).reshape(total_rows, depth)
    for k in range(depth // HEAD_SIZE):
        cols = slice(k * HEAD_SIZE, (k + 1) * HEAD_SIZE)
        normed[:, cols] = (x[:, cols] * gain[k:k + 1, :].astype(jnp.float32)).astype(jnp.bfloat16)
    squares = jnp.broadcast_to(jnp.sum(x * x, axis=1, keepdims=True), (total_rows, HEAD_SIZE))

    def put(part, start):
        width = part.shape[1]
        for j in range(n):
            for b in range(batches):
                send[j, b * here:(b + 1) * here, start:start + width] = part[
                    b * rows + j * here:b * rows + (j + 1) * here, :
                ]

    def put_halves(start, width):
        for j in range(n):
            for b in range(batches):
                at = slice(b * rows + j * here, b * rows + (j + 1) * here)
                send[j, b * here:(b + 1) * here, start:start + width] = (
                    acc[at, :width] + acc[at, width:2 * width]
                )

    def stage(start):
        return sum(start >= begin for begin in starts[1:] + [q_width])

    def shift(start, width):
        cols = pl.ds(start, width)
        def one(d):
            pltpu.make_async_remote_copy(
                src_ref=send.at[to(d), :, cols], dst_ref=recv.at[me, :, cols],
                send_sem=qs_sem, recv_sem=qr_sem.at[stage(start)],
                device_id={"gx": to(d)}, device_id_type=MESH,
            ).start()
        each(one)

    def arrived(c, start, width):
        drain(recv.at[pl.ds(0, n - 1), :, pl.ds(start, width)], qr_sem.at[c])

    def summed(start, width):
        cols = pl.ds(start, width)
        def add(d, acc):
            return acc + recv[to(d), :, cols]
        return lax.fori_loop(1, n, add, send[me, :, cols], unroll=n <= 8)

    side = kv_width + HEAD_SIZE
    take(0)
    middle = depth // 2
    for k in range(2):
        ks = slice(k * middle, (k + 1) * middle)
        acc[:, k * kv_width:(k + 1) * kv_width] = jnp.dot(
            normed[:, ks], wk[ks], preferred_element_type=jnp.float32
        )
    put_halves(q_width, kv_width)
    put(squares, q_width + kv_width)
    i = 1
    for c in range(nc):
        for k, (begin, end) in enumerate(splits[c]):
            take(i)
            i += 1
            narrow = q_widths[c] == 2 * HEAD_SIZE
            half = q_widths[c] if narrow else q_widths[c] // 2
            size = (end - begin) // 2 if narrow else end - begin
            for m in range(2):
                at = 0 if narrow else m * half
                ks = slice(begin + m * size, begin + (m + 1) * size) if narrow else slice(begin, end)
                piece = jnp.dot(
                    normed[:, ks], wq[ks, q_starts[c] + at:q_starts[c] + at + half],
                    preferred_element_type=jnp.float32,
                )
                into = slice(m * half, (m + 1) * half)
                if k > 0:
                    piece = piece + acc[:, into]
                if narrow or k < len(splits[c]) - 1:
                    acc[:, into] = piece
                else:
                    put(piece, q_starts[c] + at)
        if narrow:
            put_halves(q_starts[c], half)
        if c == 0:
            pl.semaphore_wait(barrier, n - 1 + ny - 1)
            shift(q_width, side)
        shift(q_starts[c], q_widths[c])

    small[2].wait()
    small[3].wait()
    lane = lax.broadcasted_iota(jnp.int32, (local_rows, HEAD_SIZE), 1)
    row = lax.broadcasted_iota(jnp.int32, (local_rows, HEAD_SIZE), 0)
    place = jnp.zeros((local_rows, HEAD_SIZE), jnp.float32)
    for r in range(local_rows):
        place = jnp.where(row == r, lens[r // here, r % here].astype(jnp.float32), place)
    angle = place * freq[...]
    cosine = jnp.cos(angle)
    sine = jnp.sin(angle)
    sine = jnp.where(lane < HEAD_SIZE // 2, -sine, sine)

    def rotate(v):
        return v * cosine + pltpu.roll(v, HEAD_SIZE // 2, 1) * sine

    block_rows = wide_s.shape[1]
    blocks = 2 * positions // block_rows
    half_rows = block_rows // 2

    def divide(r):
        lanes = slice((r % 2) * HEAD_SIZE, (r % 2 + 1) * HEAD_SIZE)
        for t in range(blocks):
            start = (r * blocks + t) * block_rows
            wide = wide_s.at[t % 2]
            wide[...] = kv[start:start + block_rows, :].astype(jnp.float32)
            at = slice(t * half_rows, (t + 1) * half_rows)
            keys[r // 2, at, lanes] = wide[pl.ds(0, half_rows, stride=2), :].astype(jnp.bfloat16)
            values[r // 2, at, lanes] = wide[pl.ds(1, half_rows, stride=2), :].astype(jnp.bfloat16)

    def prepare(c):
        hc = phases[c]
        arrived(c, starts[c], widths[c])
        block = summed(starts[c], widths[c])
        for h in range(hc):
            q_s[pl.ds(h, local_rows, stride=hc), :] = rotate(
                block[:, h * HEAD_SIZE:(h + 1) * HEAD_SIZE] * scale
            )

    for r in range(local_rows // 2):
        take(i)
        i += 1
        divide(r)
    wo_copy(0).start()
    arrived(last + 1, q_width, side)
    tail = summed(q_width, side)
    scale = lax.rsqrt(tail[:, kv_width:] / MODEL_WIDTH + 1e-05)
    rkey = rotate(tail[:, :HEAD_SIZE] * scale)
    value_new = tail[:, HEAD_SIZE:2 * HEAD_SIZE] * scale
    prepare(0)
    for r in range(local_rows // 2, local_rows):
        take(i)
        i += 1
        if r == local_rows - 1:
            for c in range(1, last + 1):
                wo_copy(c).start()
        divide(r)
    inv_root = np.float32(1.0 / np.sqrt(np.float32(HEAD_SIZE)))

    def spread(c):
        cols = pl.ds(starts[c], widths[c])
        def one(d):
            pltpu.make_async_remote_copy(
                src_ref=att_send.at[:, cols], dst_ref=att_recv.at[me, :, cols],
                send_sem=as_sem, recv_sem=ar_sem.at[c],
                device_id={"gx": to(d)}, device_id_type=MESH,
            ).start()
        each(one)

    for c in range(last + 1):
        hc = phases[c]
        if c > 0:
            prepare(c)
        column = lax.broadcasted_iota(jnp.int32, (2 * hc, positions), 1)
        first = lax.broadcasted_iota(jnp.int32, (2 * hc, HEAD_SIZE), 0) < hc
        first_wide = lax.broadcasted_iota(jnp.int32, (2 * hc, positions), 0) < hc

        def pair_rows(v, p):
            shape = (2 * hc, v.shape[1])
            return jnp.where(
                first,
                jnp.broadcast_to(v[2 * p:2 * p + 1], shape),
                jnp.broadcast_to(v[2 * p + 1:2 * p + 2], shape),
            )

        weighed = []
        for p in range(pairs):
            query = q_s[p * 2 * hc:(p + 1) * 2 * hc, :].astype(jnp.bfloat16).astype(jnp.float32)
            both = jnp.concatenate(
                [jnp.where(first, query, 0.0), jnp.where(first, 0.0, query)], axis=1
            ).astype(jnp.bfloat16)
            scores = jnp.concatenate(
                [
                    lax.dot_general(
                        both, keys[p, at:at + positions // 2], (((1,), (1,)), ((), ())),
                        preferred_element_type=jnp.float32,
                    )
                    for at in (0, positions // 2)
                ],
                axis=1,
            ) * inv_root
            r = 2 * p
            limit = jnp.where(
                first_wide, lens[r // here, r % here], lens[(r + 1) // here, (r + 1) % here]
            )
            scores = jnp.where(column < limit, scores, -1e30)
            new_score = jnp.sum(query * pair_rows(rkey, p), axis=1, keepdims=True) * inv_root
            top = jnp.maximum(jnp.max(scores, axis=1, keepdims=True), new_score)
            weights = jnp.exp(scores - top)
            new_weight = jnp.exp(new_score - top)
            total = jnp.sum(weights, axis=1, keepdims=True) + new_weight
            weighed.append((weights.astype(jnp.bfloat16), new_weight, total))
        for p in range(pairs):
            weights, new_weight, total = weighed[p]
            mixed = sum(
                jnp.dot(
                    weights[:, at:at + positions // 2], values[p, at:at + positions // 2],
                    preferred_element_type=jnp.float32,
                )
                for at in (0, positions // 2)
            )
            mixed = jnp.where(first, mixed[:, :HEAD_SIZE], mixed[:, HEAD_SIZE:])
            o_s[p * 2 * hc:(p + 1) * 2 * hc, :] = (
                mixed + new_weight * pair_rows(value_new, p)
            ) / total
        for h in range(hc):
            cols = slice(starts[c] + h * HEAD_SIZE, starts[c] + (h + 1) * HEAD_SIZE)
            att_send[:, cols] = o_s[pl.ds(h, local_rows, stride=hc), :].astype(jnp.bfloat16)
        spread(c)

    partner = my + 1 - 2 * lax.rem(my, 2)
    far = lax.rem(my + 2, 4)
    far_leader = far + 1 - lax.rem(far, 2)
    far_other = far + 1 - 2 * lax.rem(far, 2)
    final = len(outs) - 1
    final_cols = pl.ds(*outs[final])
    early_cols = pl.ds(0, outs[final][0])

    def hand(o, slot, target):
        cols = pl.ds(*outs[o])
        return pltpu.make_async_remote_copy(
            src_ref=y_send.at[:, cols], dst_ref=y_recv.at[slot, :, cols],
            send_sem=ys_sem.at[o // final if final else 1], recv_sem=yr_sem.at[o],
            device_id={"gy": target}, device_id_type=MESH,
        )

    def give(o):
        cols = pl.ds(*outs[o])
        return pltpu.make_async_remote_copy(
            src_ref=out.at[:, :, cols], dst_ref=out.at[:, :, cols],
            send_sem=out_sem, recv_sem=out_sem,
            device_id={"gy": partner}, device_id_type=MESH,
        )

    def product(o, fs, xc):
        start, width = outs[o]
        for at in (start, start + width // 2):
            part = slice(at, at + width // 2)
            yield part, jnp.dot(xc, wo[fs, part], preferred_element_type=jnp.float32)

    for c in range(last + 1):
        fs = slice(starts[c], starts[c] + widths[c])
        drain(att_recv.at[pl.ds(0, n - 1), :, pl.ds(starts[c], widths[c])], ar_sem.at[c])
        att_recv[me, :, fs] = att_send[:, fs]
        for j in range(n):
            block = att_recv[j, :, fs].astype(jnp.float32)
            for b in range(batches):
                x_s[b * rows + j * here:b * rows + (j + 1) * here, :widths[c]] = block[
                    b * here:(b + 1) * here, :
                ]
        xc = x_s[:, :widths[c]].astype(jnp.bfloat16)
        wo_copy(c).wait()
        if c < last:
            for o in range(len(outs)):
                for part, y in product(o, fs, xc):
                    ybuf[:, part] = y + ybuf[:, part] if c > 0 else y

    for o in range(len(outs)):
        for part, y in product(o, fs, xc):
            y_send[:, part] = (y + ybuf[:, part]).astype(jnp.bfloat16)
        if o < final:
            hand(o, 1 - lax.rem(my, 2), far_leader).start()
        else:
            hand(o, 0, far).start()
            hand(o, 1, far_other).start()
            hand(o, 2, partner).start()

    def total(o):
        cols = slice(outs[o][0], outs[o][0] + outs[o][1])
        drain(y_recv.at[:, :, cols], yr_sem.at[o])
        parts = [y_recv[slot, :, cols].astype(jnp.float32) for slot in range(3)]
        y = (y_send[:, cols].astype(jnp.float32) + parts[0]) + (parts[1] + parts[2])
        y = y.reshape(batches, rows, outs[o][1])
        out[:, :, cols] = (tok[:, :, cols].astype(jnp.float32) + y).astype(jnp.bfloat16)

    if final:
        @pl.when(leader)
        def _():
            for o in range(final):
                total(o)
                give(o).start()

        @pl.when(follower)
        def _():
            for o in range(final):
                hand(o, 2, partner).start()

    total(final)
    if final:
        @pl.when(leader)
        def _():
            drain(y_send.at[:, early_cols], ys_sem.at[0])

        @pl.when(follower)
        def _():
            drain(y_recv.at[0:2, :, early_cols], ys_sem.at[0])

        drain(out.at[:, :, early_cols], out_sem)
    drain(y_recv.at[:, :, final_cols], ys_sem.at[1])
    drain(send.at[pl.ds(0, n - 1)], qs_sem)
    drain(att_recv.at[pl.ds(0, n - 1)], as_sem)


def local(n, ny, tokens, lengths, norm_gain, w_query, key_value_weight, w_out, cache):
    batches, rows, depth = tokens.shape
    here = rows // n
    local_rows = batches * here
    q_width = w_query.shape[1]
    kv_heads = key_value_weight.shape[1]
    kv_width = kv_heads * key_value_weight.shape[2]
    assert kv_heads == 1 and ny == 4 and local_rows % 2 == 0
    heads = q_width // HEAD_SIZE
    out_width = w_out.shape[1]
    quarter = heads // 4
    chunks = (quarter,) * 3 + (quarter // 2,) * 2
    phases = (2 * quarter, 2 * quarter)
    cuts = []
    for c, width in enumerate(chunks):
        parts = max(1, depth * width * HEAD_SIZE >> 20)
        size = depth // parts
        cut = [(k * size, (k + 1) * size) for k in range(parts)]
        if c == len(chunks) - 1 and size % 512 == 0:
            begin, end = cut.pop()
            middle = begin + (end - begin) * 3 // 4
            cut += [(begin, middle), (middle, end)]
        cuts.append(cut)
    ahead = 6
    blocks = (2, 3, 3)
    eighth = out_width // 8
    outs = [(0, out_width)]
    if eighth % (2 * HEAD_SIZE) == 0:
        outs = [(sum(blocks[:o]) * eighth, blocks[o] * eighth) for o in range(len(blocks))]
    freq = np.float32(ROPE_BASE) ** (
        -2.0 * np.arange(HEAD_SIZE // 2, dtype=np.float32) / HEAD_SIZE
    )
    freq = np.concatenate([freq, freq]).astype(np.float32)[None, :]
    positions = cache.shape[2]
    interleaved = cache.reshape(local_rows * positions * 2, HEAD_SIZE)
    hbm = pl.BlockSpec(memory_space=pltpu.HBM)
    f32, bf16 = jnp.float32, jnp.bfloat16
    dma = pltpu.SemaphoreType.DMA
    total_rows = batches * rows
    wide = q_width + kv_width + HEAD_SIZE
    most = max(phases)
    return pl.pallas_call(
        functools.partial(kernel, n, ny, chunks, cuts, phases, ahead, outs),
        out_shape=pltpu.VMEM(tokens.shape, bf16),
        in_specs=[hbm] * 8,
        out_specs=pl.BlockSpec(memory_space=pltpu.VMEM),
        scratch_shapes=[
            pltpu.SMEM(lengths.shape, jnp.int32),
            pltpu.VMEM(tokens.shape, bf16),
            pltpu.VMEM((depth // HEAD_SIZE, HEAD_SIZE), bf16),
            pltpu.VMEM((1, HEAD_SIZE), f32),
            pltpu.VMEM(w_query.shape, bf16),
            pltpu.VMEM((depth, kv_width), bf16),
            pltpu.VMEM(w_out.shape, bf16),
            pltpu.VMEM(interleaved.shape, bf16),
            pltpu.VMEM((total_rows, depth), bf16),
            pltpu.VMEM((total_rows, most * HEAD_SIZE), f32),
            pltpu.VMEM((2, positions, HEAD_SIZE), f32),
            pltpu.VMEM((local_rows // 2, positions, 2 * HEAD_SIZE), bf16),
            pltpu.VMEM((local_rows // 2, positions, 2 * HEAD_SIZE), bf16),
            pltpu.VMEM((n, local_rows, wide), f32),
            pltpu.VMEM((n, local_rows, wide), f32),
            pltpu.VMEM((local_rows * most, HEAD_SIZE), f32),
            pltpu.VMEM((local_rows * most, HEAD_SIZE), f32),
            pltpu.VMEM((local_rows, q_width), bf16),
            pltpu.VMEM((n, local_rows, q_width), bf16),
            pltpu.VMEM((total_rows, most * HEAD_SIZE), f32),
            pltpu.VMEM((total_rows, out_width), f32),
            pltpu.VMEM((total_rows, out_width), bf16),
            pltpu.VMEM((3, total_rows, out_width), bf16),
            dma((4,)), dma((ahead,)), dma, dma((len(phases) + 1,)),
            dma, dma((len(phases),)), dma((2,)), dma((len(outs),)), dma,
        ],
        compiler_params=pltpu.CompilerParams(
            collective_id=0, has_side_effects=True, vmem_limit_bytes=67043328 - 2 * tokens.size
        ),
    )(
        lengths, tokens, norm_gain.reshape(depth // HEAD_SIZE, HEAD_SIZE), jnp.asarray(freq),
        w_query, key_value_weight.reshape(depth, kv_width), w_out, interleaved,
    )


def solution(mesh):
    placed = (
        P(None, "groups", "gx"),
        P(None, ("groups", "gx")),
        P("gx"),
        P("gx", "gy"),
        P("gx", "gy", None),
        P("gy", "gx"),
        P(None, ("groups", "gx"), None, "gy", None, None),
    )
    return jax.shard_map(
        functools.partial(local, mesh.shape["gx"], mesh.shape["gy"]),
        mesh=mesh, in_specs=placed, out_specs=P(None, "groups", "gx"), check_vma=False,
    )
```
